256 devices in a mesh: row: 8 (over y, z_lo), col: 4 (over z_hi), depth: 8 (over x, core).
Axes of the slice: x: 4, y: 4, z: 8 (z_hi: 4, z_lo: 2; z = z_hi * 2 + z_lo), core: 2. Of those that a mesh axis runs over, the one named last changes fastest.
Arguments:
- grad_out: bfloat16 [2048, 6144], P('depth', 'col'), may hold values from -6 to 6
- pre_act: bfloat16 [2048, 24576], P('depth', 'row'), may hold values from -8 to 8
- down_weight: bfloat16 [24576, 6144], P(('row', 'depth'), 'col'), may hold values from -0.109375 to 0.109375
Outputs:
- grad_pre: bfloat16 [2048, 24576], P('depth', 'row')
- grad_weight: bfloat16 [24576, 6144], P(('row', 'depth'), 'col')
The draws below stay inside these ranges and needn't reach their ends.
All inputs are finite; a program needn't handle non-finite values.
Results may differ from the reference program's by a relative error of at most 0.0066.
Values may be sent and summed in bfloat16 or wider, within the bound.
A program may use at most 64 MiB of HBM per device.

```python
import jax
import jax.numpy as jnp

D = 6144
FF = 24576
TOKENS = 2048


def with_spikes(values, rng, source, target, shards_of, factor):
    owner, partner = [(jnp.arange(values.shape[dim]) // (values.shape[dim] // shards_of)).reshape([-1 if axis == dim else 1 for axis in range(values.ndim)]) for dim in (source, target)]
    chosen = jax.random.permutation(rng, shards_of)[partner]
    strong = (owner == chosen) | (owner == (partner + shards_of // 2) % shards_of)
    return jnp.where(strong, factor * values, values)


def levels(stream_key, extent, cuts, low, largest):
    gain, own = 1.0, jax.random.fold_in(stream_key, 6)
    for position, parts in cuts:
        heights = jnp.exp(jax.random.uniform(jax.random.fold_in(own, position), (parts,), jnp.float32, low / len(cuts), largest / len(cuts)))
        gain = gain * jnp.repeat(heights, extent[position] // parts).reshape([-1 if axis == position else 1 for axis in range(len(extent))])
    return gain


def scatter_about(stream_key, dims, spread, bound, shards=(), held_as=jnp.bfloat16):
    entries = spread * jax.random.normal(stream_key, dims, jnp.float32)
    if shards:
        entries = entries * levels(stream_key, dims, shards, -0.22, 0.18)
    return jnp.clip(entries, -bound, bound).astype(held_as)


def gaussian_with(key, dims, spread, reach, pieces, heavy, held_as=jnp.bfloat16):
    drawn = spread * jax.random.normal(key, dims, jnp.float32)
    if pieces:
        drawn = drawn * levels(key, dims, pieces, -0.22, 0.18)
    return jnp.clip(with_spikes(drawn, jax.random.fold_in(key, 3), *heavy), -reach, reach).astype(held_as)


def setup_inputs(seed: int = 0) -> dict:
    arg_keys = jax.random.split(jax.random.key(seed), 4)
    grad_out = scatter_about(arg_keys[0], (TOKENS, D), 1.0, 6.0, ((0, 8), (1, 4)))
    pre_act = gaussian_with(arg_keys[1], (TOKENS, FF), 1.5, 8.0, ((0, 8), (1, 8)), (0, 1, 8, 2.0))
    down_weight = gaussian_with(arg_keys[2], (FF, D), FF ** -0.5, 0.109375, ((0, 64), (1, 4)), (1, 0, 64, 4.0))
    return dict(grad_out=grad_out, pre_act=pre_act, down_weight=down_weight)


sqrt_two_pi = 0.7978845608028654
cubic_coeff = 0.044715

def gelu_value(preact):
    tangent = jnp.tanh(sqrt_two_pi * (preact + cubic_coeff * preact * preact * preact))
    return 0.5 * preact * (1.0 + tangent)

def gelu_slope(preact):
    tangent = jnp.tanh(sqrt_two_pi * (preact + cubic_coeff * preact * preact * preact))
    inner = sqrt_two_pi * (1.0 + 3.0 * cubic_coeff * preact * preact)
    return 0.5 * (1.0 + tangent) + 0.5 * preact * (1.0 - tangent * tangent) * inner

def reference(grad_out, pre_act, down_weight):
    widened = pre_act.astype(jnp.float32)
    activation = gelu_value(widened).astype(jnp.bfloat16)
    backward = jnp.dot(grad_out, down_weight.T, preferred_element_type=jnp.float32)
    grad_pre = (backward * gelu_slope(widened)).astype(jnp.bfloat16)
    grad_weight = jnp.dot(activation.T, grad_out, preferred_element_type=jnp.float32).astype(jnp.bfloat16)
    return (grad_pre, grad_weight)
```

```python
import jax
import jax.numpy as jnp
from jax import lax
from jax.experimental import pallas as pl
from jax.experimental.pallas import tpu as pltpu
from jax.sharding import PartitionSpec as P

sqrt_two_pi = 0.7978845608028654
cubic_coeff = 0.044715
MESH = pl.DeviceIdType.MESH
bf16, f32 = jnp.bfloat16, jnp.float32


def gelu_value(preact):
    tangent = jnp.tanh(sqrt_two_pi * (preact + cubic_coeff * preact * preact * preact))
    return 0.5 * preact * (1.0 + tangent)


def gelu_slope(preact):
    tangent = jnp.tanh(sqrt_two_pi * (preact + cubic_coeff * preact * preact * preact))
    inner = sqrt_two_pi * (1.0 + 3.0 * cubic_coeff * preact * preact)
    return 0.5 * (1.0 + tangent) + 0.5 * preact * (1.0 - tangent * tangent) * inner


def kernel(
    g_hbm, p_hbm, w_hbm, go_hbm, gw_hbm,
    gbuf, pbuf, wbuf, csend, crecv, keep_a, keep_b, keep_own, dsend, ebuf, act_t, gw_buf,
    load_sem, a_recv, p_recv, c_recv, d_recv, e_recv, out_sem,
    a_send, r_send, rx_send, p_send, c_send, d_send, e_send, f_send,
):
    row, col, dep = lax.axis_index("row"), lax.axis_index("col"), lax.axis_index("depth")
    x, core = dep // 2, dep % 2
    other = 1 - core
    chunk = g_hbm.shape[1]
    wide = wbuf.shape[0]
    right, left, far = (x + 1) % 4, (x + 3) % 4, (x + 2) % 4
    up, down = (col + 1) % 4, (col + 3) % 4
    order = [(col + 2) % 4, up, down, col]
    source = {0: x, 1: right, 2: far, 3: left}
    pending = []

    def at_depth(d):
        return (row, col, d)

    def at_col(c):
        return (row, c, dep)

    def send(src, dst, send_sem, recv_sem, device):
        copy = pltpu.make_async_remote_copy(
            src_ref=src, dst_ref=dst, send_sem=send_sem, recv_sem=recv_sem, device_id=device, device_id_type=MESH
        )
        copy.start()
        pending.append(copy)

    def arrived(dst, recv_sem):
        pltpu.make_async_copy(dst, dst, recv_sem).wait()

    loads = {}
    for i, q in enumerate(order):
        loads["g", i] = pltpu.make_async_copy(g_hbm.at[q], gbuf.at[x, q, core], load_sem.at[0, i])
        loads["g", i].start()
    loads["w"] = pltpu.make_async_copy(w_hbm, wbuf, load_sem.at[2, 0])
    loads["w"].start()

    def hidden(d):
        return pl.ds(pl.multiple_of(d * wide, 128), wide)

    for i, q in enumerate(order):
        loads["p", i] = pltpu.make_async_copy(p_hbm.at[q, :, hidden(dep)], pbuf.at[x, q, core], load_sem.at[1, i])
        loads["p", i].start()

    barrier = pltpu.get_barrier_semaphore()
    for t in range(1, 8):
        pl.semaphore_signal(barrier, inc=1, device_id=at_depth((dep + t) % 8), device_id_type=MESH)
    for c in (up, down):
        pl.semaphore_signal(barrier, inc=1, device_id=at_col(c), device_id_type=MESH)
    pl.semaphore_wait(barrier, 9)

    def send_pre(i):
        q = order[i]
        for t in range(1, 8):
            d = (dep + t) % 8
            send(p_hbm.at[q, :, hidden(d)], pbuf.at[x, q, core], p_send.at[i, t], p_recv.at[x, q, core], at_depth(d))

    for i, q in enumerate(order):
        loads["g", i].wait()
        mine = gbuf.at[x, q, core]
        for t, d in enumerate((2 * x + other, 2 * right + core, 2 * left + core)):
            send(mine, mine, a_send.at[i, t], a_recv.at[x, q, core], at_depth(d))
        if i == 2:
            send_pre(3)

    def relay(r, i, onward):
        part = gbuf.at[source[r], order[i], core]
        sem = a_recv.at[source[r], order[i], core]
        arrived(part, sem)
        send(part, part, r_send.at[r, i], sem, at_depth(2 * x + other))
        if onward is not None:
            send(part, part, rx_send.at[i], sem, at_depth(2 * onward + core))

    def partner_part(r, i):
        arrived(gbuf.at[source[r], order[i], other], a_recv.at[source[r], order[i], other])

    def to_col(r, kind, way):
        send(
            csend.at[r, kind, way], crecv.at[r, kind, way], c_send.at[r, kind, way], c_recv.at[r, kind, way],
            at_col((up, down)[way]),
        )

    def group(r, i):
        rows = gbuf[source[r], order[i]].reshape(2 * chunk, gbuf.shape[4])
        part = lax.dot_general(rows, wbuf[...], (((1,), (1,)), ((), ())), preferred_element_type=f32)
        low, high = part[:chunk], part[chunk:]
        if i == 0:
            csend[r, 0, 0] = low.astype(bf16)
            csend[r, 0, 1] = high.astype(bf16)
            to_col(r, 0, 0)
            to_col(r, 0, 1)
        elif i == 1:
            csend[r, 1, 0] = high.astype(bf16)
            keep_a[r] = low
            to_col(r, 1, 0)
        elif i == 2:
            csend[r, 1, 1] = low.astype(bf16)
            keep_b[r] = high
            to_col(r, 1, 1)
        else:
            keep_own[r, 0] = low
            keep_own[r, 1] = high

    def combine(r, way):
        arrived(crecv.at[r, 0, way], c_recv.at[r, 0, way])
        kept = (keep_a, keep_b)[way][r]
        csend[r, 2, way] = (kept + crecv[r, 0, way].astype(f32)).astype(bf16)
        to_col(r, 2, way)

    def finish(r):
        for kind in (1, 2):
            for way in (0, 1):
                arrived(crecv.at[r, kind, way], c_recv.at[r, kind, way])
        s = source[r]
        if r == 0:
            loads["p", 3].wait()
            arrived(pbuf.at[s, col, other], p_recv.at[s, col, other])
        else:
            for k in (0, 1):
                arrived(pbuf.at[s, col, k], p_recv.at[s, col, k])
        for k in (0, 1):
            total = keep_own[r, k] + crecv[r, 2, k].astype(f32) + crecv[r, 1, 1 - k].astype(f32)
            dsend[r, k] = (total * gelu_slope(pbuf[s, col, k].astype(f32))).astype(bf16)
        if r == 0:
            ebuf[col, dep] = dsend[0, core]
            send(
                dsend.at[0, other], ebuf.at[col, dep], d_send.at[0, 0], d_recv.at[dep], at_depth(2 * x + other)
            )
        else:
            for k in (0, 1):
                send(dsend.at[r, k], ebuf.at[col, dep], d_send.at[r, k], d_recv.at[dep], at_depth(2 * s + k))

    outs = []

    def write_out(c, j):
        copy = pltpu.make_async_copy(ebuf.at[c, j], go_hbm.at[c, :, hidden(j)], out_sem.at[c, j])
        copy.start()
        outs.append(copy)

    def e_own(r):
        s = source[r]
        if r == 0:
            arrived(ebuf.at[col, 2 * x + other], d_recv.at[2 * x + other])
        else:
            for k in (0, 1):
                arrived(ebuf.at[col, 2 * s + k], d_recv.at[2 * s + k])
        for k in (0, 1):
            j = 2 * s + k
            for way, c in enumerate((up, down)):
                send(ebuf.at[col, j], ebuf.at[col, j], e_send.at[r, k, way], e_recv.at[way, j], at_col(c))
            write_out(col, j)

    def e_forward(r):
        s = source[r]
        for k, (frm, to) in enumerate(((down, up), (up, down))):
            j = 2 * s + k
            arrived(ebuf.at[frm, j], e_recv.at[k, j])
            send(ebuf.at[frm, j], ebuf.at[frm, j], f_send.at[r, k], e_recv.at[2, j], at_col(to))
            write_out(frm, j)

    def e_rest(r):
        s = source[r]
        for k, frm in enumerate((up, down)):
            j = 2 * s + k
            arrived(ebuf.at[frm, j], e_recv.at[1 - k, j])
            write_out(frm, j)
        for k in (0, 1):
            j = 2 * s + k
            arrived(ebuf.at[(col + 2) % 4, j], e_recv.at[2, j])
            write_out((col + 2) % 4, j)

    def activate(r, i, wait):
        s, q = source[r], order[i]
        if wait:
            if r == 0:
                loads["p", i].wait()
                arrived(pbuf.at[s, q, other], p_recv.at[s, q, other])
            else:
                for k in (0, 1):
                    arrived(pbuf.at[s, q, k], p_recv.at[s, q, k])
        pre = pbuf[s, q].reshape(2 * chunk, wide).astype(f32)
        place = pl.ds(pl.multiple_of((4 * s + q) * 2 * chunk, 128), 2 * chunk)
        act_t[:, place] = gelu_value(pre).astype(bf16).T

    loads["w"].wait()
    for i in range(4):
        partner_part(0, i)
        group(0, i)
    combine(0, 0)
    combine(0, 1)

    for i in range(4):
        relay(3, i, right if i < 2 else None)
        relay(1, i, left if i >= 2 else None)
        for r in (3, 1):
            partner_part(r, i)
            group(r, i)
        if i == 1:
            combine(1, 0)
            combine(3, 0)
            finish(0)
        if i == 2:
            combine(1, 1)
            combine(3, 1)
            e_own(0)
    for i in (0, 2):
        relay(2, i, None)
        partner_part(2, i)
        group(2, i)
    finish(1)
    finish(3)
    send_pre(0)
    for i in (1, 3):
        relay(2, i, None)
        partner_part(2, i)
        group(2, i)
    e_forward(0)
    combine(2, 0)
    combine(2, 1)
    e_own(1)
    e_own(3)
    for r in range(4):
        if r != 2:
            activate(r, 3, False)
    finish(2)
    send_pre(1)
    send_pre(2)
    activate(2, 3, False)
    e_forward(1)
    e_forward(3)
    e_own(2)
    for i in (0, 1, 2):
        for r in range(4):
            activate(r, i, True)
        if i == 1:
            e_forward(2)
            e_rest(0)
    every_grad = gbuf.reshape(gbuf.shape[0] * 8 * chunk, gbuf.shape[4])
    tile = 256
    for n in range(gbuf.shape[4] // tile):
        cols = pl.ds(n * tile, tile)
        gw_buf[:, cols] = jnp.dot(act_t[...], every_grad[:, cols], preferred_element_type=f32).astype(bf16)
        copy = pltpu.make_async_copy(gw_buf.at[:, cols], gw_hbm.at[:, cols], load_sem.at[3, n])
        copy.start()
        outs.append(copy)
        if n == 2:
            e_rest(1)
            e_rest(3)
    e_rest(2)
    for copy in pending:
        copy.wait_send()
    for copy in outs:
        copy.wait()


def on_device(grad_out, pre_act, down_weight):
    tokens, features = grad_out.shape
    hidden = pre_act.shape[1]
    wide = down_weight.shape[0]
    chunk = tokens // 4
    any_spec = pl.BlockSpec(memory_space=pl.ANY)
    dma = pltpu.SemaphoreType.DMA
    grad_pre, grad_weight = pl.pallas_call(
        kernel,
        out_shape=(
            jax.ShapeDtypeStruct((4, chunk, hidden), bf16),
            jax.ShapeDtypeStruct((wide, features), bf16),
        ),
        in_specs=[any_spec] * 3,
        out_specs=(any_spec, any_spec),
        scratch_shapes=[
            pltpu.VMEM((4, 4, 2, chunk, features), bf16),
            pltpu.VMEM((4, 4, 2, chunk, wide), bf16),
            pltpu.VMEM((wide, features), bf16),
            pltpu.VMEM((4, 3, 2, chunk, wide), bf16),
            pltpu.VMEM((4, 3, 2, chunk, wide), bf16),
            pltpu.VMEM((4, chunk, wide), f32),
            pltpu.VMEM((4, chunk, wide), f32),
            pltpu.VMEM((4, 2, chunk, wide), f32),
            pltpu.VMEM((4, 2, chunk, wide), bf16),
            pltpu.VMEM((4, 8, chunk, wide), bf16),
            pltpu.VMEM((wide, 32 * chunk), bf16),
            pltpu.VMEM((wide, features), bf16),
            dma((4, 8)), dma((4, 4, 2)), dma((4, 4, 2)), dma((4, 3, 2)), dma((8,)), dma((3, 8)), dma((4, 8)),
            dma((4, 3)), dma((4, 4)), dma((4,)), dma((4, 8)), dma((4, 3, 2)), dma((4, 2)), dma((4, 2, 2)), dma((4, 2)),
        ],
        compiler_params=pltpu.CompilerParams(collective_id=0, has_side_effects=True),
    )(
        grad_out.reshape(4, chunk, features),
        pre_act.reshape(4, chunk, hidden),
        down_weight,
    )
    return grad_pre.reshape(tokens, hidden), grad_weight


def solution(mesh):
    placed = (P("depth", "col"), P("depth", "row"), P(("row", "depth"), "col"))
    return jax.shard_map(
        on_device,
        mesh=mesh,
        in_specs=placed,
        out_specs=(P("depth", "row"), P(("row", "depth"), "col")),
        check_vma=False,
    )
```

```python
import jax
import jax.numpy as jnp
from jax import lax
from jax.experimental import pallas as pl
from jax.experimental.pallas import tpu as pltpu
from jax.sharding import PartitionSpec as P

sqrt_two_pi = 0.7978845608028654
cubic_coeff = 0.044715
MESH = pl.DeviceIdType.MESH
bf16, f32 = jnp.bfloat16, jnp.float32


def gelu_value(preact):
    tangent = jnp.tanh(sqrt_two_pi * (preact + cubic_coeff * preact * preact * preact))
    return 0.5 * preact * (1.0 + tangent)


def gelu_slope(preact):
    tangent = jnp.tanh(sqrt_two_pi * (preact + cubic_coeff * preact * preact * preact))
    inner = sqrt_two_pi * (1.0 + 3.0 * cubic_coeff * preact * preact)
    return 0.5 * (1.0 + tangent) + 0.5 * preact * (1.0 - tangent * tangent) * inner


def kernel(
    g_hbm, p_hbm, w_hbm, go, gw,
    gbuf, pbuf, wbuf, first, csend, crecv, keep, keep_own, dsend, act_t, gw_sum,
    load_sem, a_recv, p_recv, c_recv, d_recv, e_recv,
    a_send, r_send, rx_send, p_send, c_send, d_send, e_send, f_send,
):
    row, col, dep = lax.axis_index("row"), lax.axis_index("col"), lax.axis_index("depth")
    x, core = dep // 2, dep % 2
    other = 1 - core
    chunk, features = g_hbm.shape[1:]
    wide = wbuf.shape[0]
    right, left, far = (x + 1) % 4, (x + 3) % 4, (x + 2) % 4
    up, down = (col + 1) % 4, (col + 3) % 4
    order = [(col + 2) % 4, up, down, col]
    source = {0: x, 1: right, 2: far, 3: left}
    pending = []

    def at_depth(d):
        return (row, col, d)

    def at_col(c):
        return (row, c, dep)

    def flush():
        for copy in pending:
            copy.wait_send()
        pending.clear()

    def send(src, dst, send_sem, recv_sem, device):
        copy = pltpu.make_async_remote_copy(
            src_ref=src, dst_ref=dst, send_sem=send_sem, recv_sem=recv_sem, device_id=device, device_id_type=MESH
        )
        copy.start()
        pending.append(copy)

    def arrived(dst, recv_sem):
        pltpu.make_async_copy(dst, dst, recv_sem).wait()

    def hidden(d):
        return pl.ds(pl.multiple_of(d * wide, 128), wide)

    def times_weight(rows):
        return lax.dot_general(rows, wbuf[...], (((1,), (1,)), ((), ())), preferred_element_type=f32)

    barrier = pltpu.get_barrier_semaphore()
    for c in (up, down):
        pl.semaphore_signal(barrier, inc=1, device_id=at_col(c), device_id_type=MESH)
    for t in range(1, 8):
        pl.semaphore_signal(barrier, inc=1, device_id=at_depth((dep + t) % 8), device_id_type=MESH)
    loads = [pltpu.make_async_copy(w_hbm, wbuf, load_sem.at[2, 0])]
    for i, q in enumerate(order):
        loads.append(pltpu.make_async_copy(g_hbm.at[q], gbuf.at[x, q, core], load_sem.at[0, i]))
    for i, q in enumerate(order):
        loads.append(pltpu.make_async_copy(p_hbm.at[q, :, hidden(dep)], pbuf.at[x, q, core], load_sem.at[1, i]))
    for copy in loads:
        copy.start()
    for copy in loads[:5]:
        copy.wait()

    def own_part(k):
        for i, q in enumerate(order):
            first[k, i] = times_weight(gbuf[x, q, k])
        csend[0, 0, k] = first[k, 0].astype(bf16)
        csend[0, 1, 1 - k] = first[k, 2 - k].astype(bf16)
        keep[0, k] = first[k, 1 + k]
        keep_own[0, k] = first[k, 3]

    own_part(core)
    for copy in loads[5:]:
        copy.wait()
    pl.semaphore_wait(barrier, 9)

    def to_col(r, kind, way):
        send(
            csend.at[r, kind, way], crecv.at[r, kind, way], c_send.at[r, kind, way], c_recv.at[r, kind, way],
            at_col((col + 1 + 2 * way) % 4),
        )

    def send_grad(i, devices):
        mine = gbuf.at[x, order[i], core]
        for t, d in devices:
            send(mine, mine, a_send.at[i, t], a_recv.at[x, order[i], core], at_depth(d))

    def send_pre(i, distances):
        q = order[i]
        for t in distances:
            d = (2 * ((x + t) % 4) + core) if t < 4 else (2 * ((x + t - 4) % 4) + other)
            send(p_hbm.at[q, :, hidden(d)], pbuf.at[x, q, core], p_send.at[i, t], p_recv.at[x, q, core], at_depth(d))

    partner = ((0, 2 * x + other),)
    ahead, behind = ((1, 2 * right + core),), ((2, 2 * left + core),)
    send_grad(0, ahead)
    send_grad(0, behind)
    to_col(0, 0, core)
    to_col(0, 1, other)
    for i in range(4):
        send_grad(i, partner)
    for i, j in ((1, 2), (2, 1), (3, 3)):
        send_grad(i, ahead)
        send_grad(j, behind)
    send_pre(3, (1, 3, 5, 7))
    for i in (3, 0, 1, 2):
        send_pre(i, (4,))

    def relay(r, i, onward):
        part = gbuf.at[source[r], order[i], core]
        sem = a_recv.at[source[r], order[i], core]
        arrived(part, sem)
        send(part, part, r_send.at[r, i], sem, at_depth(2 * x + other))
        if onward is not None:
            send(part, part, rx_send.at[i], sem, at_depth(2 * onward + core))

    def partner_part(r, i):
        arrived(gbuf.at[source[r], order[i], other], a_recv.at[source[r], order[i], other])

    def group(r, i):
        part = times_weight(gbuf[source[r], order[i]].reshape(2 * chunk, features))
        low, high = part[:chunk], part[chunk:]
        if i == 0:
            csend[r, 0, 0] = low.astype(bf16)
            csend[r, 0, 1] = high.astype(bf16)
            to_col(r, 0, 0)
            to_col(r, 0, 1)
        elif i == 1:
            csend[r, 1, 0] = high.astype(bf16)
            keep[r, 0] = low
            to_col(r, 1, 0)
        elif i == 2:
            csend[r, 1, 1] = low.astype(bf16)
            keep[r, 1] = high
            to_col(r, 1, 1)
        else:
            keep_own[r, 0] = low
            keep_own[r, 1] = high

    def combine(r, way):
        arrived(crecv.at[r, 0, way], c_recv.at[r, 0, way])
        csend[r, 2, way] = (keep[r, way] + crecv[r, 0, way].astype(f32)).astype(bf16)
        to_col(r, 2, way)

    def pre_arrived(r, i):
        s, q = source[r], order[i]
        if r == 0:
            arrived(pbuf.at[s, q, other], p_recv.at[s, q, other])
        else:
            for k in (0, 1):
                arrived(pbuf.at[s, q, k], p_recv.at[s, q, k])

    def finish(r):
        for kind in (1, 2):
            for way in (0, 1):
                arrived(crecv.at[r, kind, way], c_recv.at[r, kind, way])
        s = source[r]
        for k in (0, 1):
            total = keep_own[r, k] + crecv[r, 2, k].astype(f32) + crecv[r, 1, 1 - k].astype(f32)
            dsend[r, k] = (total * gelu_slope(pbuf[s, col, k].astype(f32))).astype(bf16)
        mine = go.at[col, :, hidden(dep)]
        if r == 0:
            send(dsend.at[0, other], mine, d_send.at[0, 0], d_recv.at[dep], at_depth(2 * x + other))
            go[col, :, hidden(dep)] = dsend[0, core]
        else:
            for k in (0, 1):
                send(dsend.at[r, k], mine, d_send.at[r, k], d_recv.at[dep], at_depth(2 * s + k))

    def piece(c, j):
        return go.at[c, :, hidden(j)]

    def e_own(r):
        s = source[r]
        if r == 0:
            arrived(piece(col, 2 * x + other), d_recv.at[2 * x + other])
        else:
            for k in (0, 1):
                arrived(piece(col, 2 * s + k), d_recv.at[2 * s + k])
        for k in (0, 1):
            j = 2 * s + k
            for way, c in enumerate((up, down)):
                send(piece(col, j), piece(col, j), e_send.at[r, k, way], e_recv.at[way, j], at_col(c))

    def e_forward(r):
        s = source[r]
        for k, (frm, to) in enumerate(((down, up), (up, down))):
            j = 2 * s + k
            arrived(piece(frm, j), e_recv.at[k, j])
            send(piece(frm, j), piece(frm, j), f_send.at[r, k], e_recv.at[2, j], at_col(to))

    def e_rest(r):
        s = source[r]
        for k, frm in enumerate((up, down)):
            j = 2 * s + k
            arrived(piece(frm, j), e_recv.at[1 - k, j])
        for k in (0, 1):
            j = 2 * s + k
            arrived(piece((col + 2) % 4, j), e_recv.at[2, j])

    def activate(r, i):
        s, q = source[r], order[i]
        pre = pbuf[s, q].reshape(2 * chunk, wide).astype(f32)
        place = pl.ds(pl.multiple_of((4 * s + q) * 2 * chunk, 128), 2 * chunk)
        act_t[:, place] = gelu_value(pre).astype(bf16).T

    def weight_grad(r, n):
        s, cols = source[r], pl.ds(n * 512, 512)
        span = 8 * chunk
        part = jnp.dot(
            act_t[:, pl.ds(pl.multiple_of(s * span, 128), span)],
            gbuf[s, :, :, :, cols].reshape(span, 512),
            preferred_element_type=f32,
        )
        if r == 0:
            gw_sum[:, cols] = part
        elif r == 2:
            gw[:, cols] = (gw_sum[:, cols] + part).astype(bf16)
        else:
            gw_sum[:, cols] += part

    def weight_grads(r):
        for n in range(features // 512):
            weight_grad(r, n)

    for i in range(4):
        partner_part(0, i)
    own_part(other)
    to_col(0, 0, other)
    to_col(0, 1, core)
    for i in (3, 0, 1, 2):
        pre_arrived(0, i)
        activate(0, i)
    combine(0, core)
    combine(0, other)

    def two_groups(i, j):
        relay(3, i, right if i < 2 else None)
        relay(1, j, left if j >= 2 else None)
        for r, n in ((3, i), (1, j)):
            partner_part(r, n)
            group(r, n)

    def far_groups(i, j):
        relay(2, i, None)
        relay(2, j, None)
        for n in (i, j):
            partner_part(2, n)
            group(2, n)

    two_groups(0, 0)
    weight_grads(0)
    two_groups(1, 2)
    finish(0)
    two_groups(2, 1)
    e_own(0)
    for way in (0, 1):
        combine(3, way)
        combine(1, 1 - way)
    two_groups(3, 3)
    for r in (1, 3):
        pre_arrived(r, 3)
        activate(r, 3)
    far_groups(0, 2)
    finish(3)
    finish(1)
    send_pre(3, (2, 6))
    send_pre(0, (1, 3, 5, 7))
    e_forward(0)
    far_groups(1, 3)
    combine(2, 0)
    combine(2, 1)
    e_own(1)
    e_own(3)
    pre_arrived(2, 3)
    activate(2, 3)
    finish(2)
    send_pre(1, (1, 3, 5, 7))
    send_pre(2, (1, 3, 5, 7))
    for i in (0, 1, 2):
        send_pre(i, (2, 6))
    e_forward(1)
    e_own(2)
    e_forward(3)
    for i in (0, 1, 2):
        for r in (1, 3):
            pre_arrived(r, i)
            activate(r, i)
    weight_grads(1)
    weight_grads(3)
    e_forward(2)
    e_rest(0)
    for i in (0, 1, 2):
        pre_arrived(2, i)
        activate(2, i)
    weight_grads(2)
    flush()
    e_rest(1)
    e_rest(3)
    e_rest(2)


def on_device(grad_out, pre_act, down_weight):
    tokens, features = grad_out.shape
    hidden = pre_act.shape[1]
    wide = down_weight.shape[0]
    chunk = tokens // 4
    vmem_spec = pl.BlockSpec(memory_space=pltpu.VMEM)
    dma = pltpu.SemaphoreType.DMA
    operands = (grad_out.reshape(4, chunk, features), pre_act.reshape(4, chunk, hidden), down_weight)
    grad_pre, grad_weight = pl.pallas_call(
        kernel,
        out_shape=(
            jax.ShapeDtypeStruct((4, chunk, hidden), bf16),
            jax.ShapeDtypeStruct((wide, features), bf16),
        ),
        in_specs=[pl.BlockSpec(memory_space=pl.ANY)] * 3,
        out_specs=(vmem_spec, vmem_spec),
        scratch_shapes=[
            pltpu.VMEM((4, 4, 2, chunk, features), bf16),
            pltpu.VMEM((4, 4, 2, chunk, wide), bf16),
            pltpu.VMEM((wide, features), bf16),
            pltpu.VMEM((2, 4, chunk, wide), f32),
            pltpu.VMEM((4, 3, 2, chunk, wide), bf16),
            pltpu.VMEM((4, 3, 2, chunk, wide), bf16),
            pltpu.VMEM((4, 2, chunk, wide), f32),
            pltpu.VMEM((4, 2, chunk, wide), f32),
            pltpu.VMEM((4, 2, chunk, wide), bf16),
            pltpu.VMEM((wide, 32 * chunk), bf16),
            pltpu.VMEM((wide, features), f32),
            dma((3, 4)), dma((4, 4, 2)), dma((4, 4, 2)), dma((4, 3, 2)), dma((8,)), dma((3, 8)),
            dma((4, 3)), dma((4, 4)), dma((4,)), dma((4, 8)), dma((4, 3, 2)), dma((4, 2)), dma((4, 2, 2)), dma((4, 2)),
        ],
        compiler_params=pltpu.CompilerParams(
            collective_id=0, has_side_effects=True, vmem_limit_bytes=44 * 1024 * 1024
        ),
    )(*(pltpu.with_memory_space_constraint(operand, pltpu.HBM) for operand in operands))
    return grad_pre.reshape(tokens, hidden), grad_weight


def solution(mesh):
    placed = (P("depth", "col"), P("depth", "row"), P(("row", "depth"), "col"))
    return jax.shard_map(
        on_device,
        mesh=mesh,
        in_specs=placed,
        out_specs=(P("depth", "row"), P(("row", "depth"), "col")),
        check_vma=False,
    )
```

```python
import jax
import jax.numpy as jnp
from jax import lax
from jax.experimental import pallas as pl
from jax.experimental.pallas import tpu as pltpu
from jax.sharding import PartitionSpec as P

sqrt_two_pi = 0.7978845608028654
cubic_coeff = 0.044715
MESH = pl.DeviceIdType.MESH
bf16, f32 = jnp.bfloat16, jnp.float32


def gelu_value(preact):
    tangent = jnp.tanh(sqrt_two_pi * (preact + cubic_coeff * preact * preact * preact))
    return 0.5 * preact * (1.0 + tangent)


def gelu_slope(preact):
    tangent = jnp.tanh(sqrt_two_pi * (preact + cubic_coeff * preact * preact * preact))
    inner = sqrt_two_pi * (1.0 + 3.0 * cubic_coeff * preact * preact)
    return 0.5 * (1.0 + tangent) + 0.5 * preact * (1.0 - tangent * tangent) * inner


PLAN = [
    ("P", 3, 1), ("P", 3, 3), ("A", 0, 3), ("A", 0, 0), ("A", 0, 1), ("A", 0, 2), ("C", 0, 0), ("C", 0, 1), ("X",
    3, 0), ("X", 1, 0), ("G", 3, 0), ("G", 1, 0), ("M", 0, 0), ("M", 0, 1), ("M", 0, 2), ("X", 3, 1), ("X", 1, 2),
    ("G", 3, 1), ("G", 1, 2), ("F", 0), ("X", 3, 2), ("X", 1, 1), ("G", 3, 2), ("G", 1, 1), ("O", 0), ("C", 3, 0),
    ("C", 1, 1), ("C", 3, 1), ("C", 1, 0), ("X", 3, 3), ("X", 1, 3), ("Y", 3, 3), ("Y", 1, 3), ("G", 3, 3), ("G",
    1, 3), ("A", 1, 3), ("A", 3, 3), ("X", 2, 0), ("X", 2, 2), ("G", 2, 0), ("G", 2, 2), ("F", 3), ("F", 1), ("P",
    3, 2), ("P", 0, 1), ("P", 0, 3), ("W", 0), ("X", 2, 1), ("X", 2, 3), ("Y", 2, 3), ("G", 2, 1), ("G", 2, 3),
    ("C", 2, 0), ("C", 2, 1), ("O", 1), ("O", 3), ("A", 2, 3), ("F", 2), ("P", 1, 1), ("P", 1, 3), ("P", 2, 1),
    ("P", 2, 3), ("P", 0, 2), ("P", 1, 2), ("P", 2, 2), ("W", 1), ("O", 2), ("W", 3), ("A", 1, 0), ("A", 1, 1),
    ("A", 1, 2), ("A", 3, 0), ("A", 3, 1), ("A", 3, 2), ("M", 1, 0), ("M", 1, 1), ("M", 1, 2), ("M", 3, 0), ("M",
    3, 1), ("M", 3, 2), ("W", 2), ("R", 0), ("A", 2, 0), ("A", 2, 1), ("A", 2, 2), ("M", 2, 0), ("M", 2, 1), ("M",
    2, 2), ("R", 1), ("R", 3), ("R", 2),
]


WHOLE = (0, 1, 2)

def kernel(
    g_hbm, p_hbm, w_hbm, go, gw,
    gbuf, pbuf, wbuf, first, csend, crecv, keep, keep_own, dsend, act_t, gw_sum, gw_buf,
    load_sem, out_sem, s_recv, a_recv, p_recv, c_recv, d_recv, e_recv, sent,
):
    row, col, dep = lax.axis_index("row"), lax.axis_index("col"), lax.axis_index("depth")
    x, core = dep // 2, dep % 2
    other = 1 - core
    part_rows, features = g_hbm.shape[2:]
    chunk = 2 * part_rows
    wide = wbuf.shape[0]
    y = row // 2
    half = y % 2
    north, south = (row + 2) % 8, (row + 6) % 8
    right, left, far = (x + 1) % 4, (x + 3) % 4, (x + 2) % 4
    up, down = (col + 1) % 4, (col + 3) % 4
    order = [(col + 2) % 4, up, down, col]
    source = {0: x, 1: right, 2: far, 3: left}
    local = []

    def at_depth(d):
        return (row, col, d)

    def at_col(c):
        return (row, c, dep)

    GRAD, PRE, SUM, SHARE, SPREAD = range(5)

    def send(kind, src, dst, recv_sem, device):
        pltpu.make_async_remote_copy(
            src_ref=src, dst_ref=dst, send_sem=sent.at[kind], recv_sem=recv_sem, device_id=device, device_id_type=MESH
        ).start()

    def arrived(dst, recv_sem):
        pltpu.make_async_copy(dst, dst, recv_sem).wait()

    def hidden(d):
        return pl.ds(pl.multiple_of(d * wide, 128), wide)

    def times_weight(rows):
        return lax.dot_general(rows, wbuf[...], (((1,), (1,)), ((), ())), preferred_element_type=f32)

    barrier = pltpu.get_barrier_semaphore()
    for c in (up, down):
        pl.semaphore_signal(barrier, inc=1, device_id=at_col(c), device_id_type=MESH)
    for t in range(1, 8):
        pl.semaphore_signal(barrier, inc=1, device_id=at_depth((dep + t) % 8), device_id_type=MESH)
    for n in (north, south):
        pl.semaphore_signal(barrier, inc=1, device_id=(n, col, dep), device_id_type=MESH)
    loads = [
        pltpu.make_async_copy(w_hbm, wbuf, load_sem.at[0]),
        pltpu.make_async_copy(g_hbm, gbuf.at[x, :, core], load_sem.at[1]),
        pltpu.make_async_copy(p_hbm.at[:, :, hidden(dep)], pbuf.at[x, :, core], load_sem.at[2]),
    ]
    for copy in loads:
        copy.start()
    loads[0].wait()
    loads[1].wait()

    def own_part(k):
        rows = gbuf[x, :, k].reshape(4 * chunk, features)
        first[k] = times_weight(rows).reshape(4, chunk, wide)
        csend[0, 0, k] = first[k, order[0]].astype(bf16)
        csend[0, 1, 1 - k] = first[k, (col + 3 + 2 * k) % 4].astype(bf16)
        keep[0, k] = first[k, (col + 1 + 2 * k) % 4]
        keep_own[0, k] = first[k, col]

    own_part(core)
    loads[2].wait()
    pl.semaphore_wait(barrier, 11)

    def to_col(r, kind, way):
        sem = c_recv.at[r, way] if kind == 0 else c_recv.at[r, 2]
        send(SUM, csend.at[r, kind, way], crecv.at[r, kind, way], sem, at_col((col + 1 + 2 * way) % 4))

    def send_grad(i, r, d):
        mine = gbuf.at[x, order[i], core] if i in WHOLE else gbuf.at[x, order[i], core, half]
        send(GRAD, mine, mine, a_recv.at[r - 1, i, 0], at_depth(d))

    def send_pre(i, t):
        q = order[i]
        sem = p_recv.at[(4 - t) % 4, 0 if i == 3 else 1]
        for d in (2 * ((x + t) % 4) + core, 2 * ((x + t) % 4) + other)[0 if t else 1 :]:
            send(PRE, p_hbm.at[q, :, hidden(d)], pbuf.at[x, q, core], sem, at_depth(d))

    send_grad(0, 3, 2 * right + core)
    send_grad(0, 1, 2 * left + core)
    to_col(0, 0, core)
    to_col(0, 1, other)
    mine = gbuf.at[x, :, core]
    send(GRAD, mine, mine, s_recv, at_depth(2 * x + other))
    for i, j in ((1, 2), (2, 1), (3, 3)):
        send_grad(i, 3, 2 * right + core)
        send_grad(j, 1, 2 * left + core)
    for i in (3, 0, 1, 2):
        send_pre(i, 0)

    def from_x(r, i):
        part, sem = gbuf.at[source[r], order[i], core], a_recv.at[r - 1, i]
        if i not in WHOLE:
            part = part.at[half]
        arrived(part, sem.at[0])
        from_left = r == 3 or (r == 2 and i < 2)
        if i not in WHOLE:
            send(GRAD, part, part, sem.at[1], (north if from_left else south, col, dep))
        send(GRAD, part, part, sem.at[2], at_depth(2 * x + other))
        if r == 3 and i < 2:
            send(GRAD, part, part, a_recv.at[1, i, 0], at_depth(2 * right + core))
        if r == 1 and i >= 2:
            send(GRAD, part, part, a_recv.at[1, i, 0], at_depth(2 * left + core))

    def from_y(r, i):
        if i in WHOLE:
            return
        part, sem = gbuf.at[source[r], order[i], core, 1 - half], a_recv.at[r - 1, i]
        arrived(part, sem.at[1])
        send(GRAD, part, part, sem.at[2], at_depth(2 * x + other))

    def group(r, i):
        s, q = source[r], order[i]
        arrived(gbuf.at[s, q, other], a_recv.at[r - 1, i, 2])
        part = times_weight(gbuf[s, q].reshape(2 * chunk, features))
        low, high = part[:chunk], part[chunk:]
        if i == 0:
            csend[r, 0, 0] = low.astype(bf16)
            csend[r, 0, 1] = high.astype(bf16)
            to_col(r, 0, 0)
            to_col(r, 0, 1)
        elif i == 1:
            csend[r, 1, 0] = high.astype(bf16)
            keep[r, 0] = low
            to_col(r, 1, 0)
        elif i == 2:
            csend[r, 1, 1] = low.astype(bf16)
            keep[r, 1] = high
            to_col(r, 1, 1)
        else:
            keep_own[r, 0] = low
            keep_own[r, 1] = high

    def combine(r, way):
        arrived(crecv.at[r, 0, way], c_recv.at[r, way])
        csend[r, 2, way] = (keep[r, way] + crecv[r, 0, way].astype(f32)).astype(bf16)
        to_col(r, 2, way)

    seen = set()

    def pre_arrived(r, i):
        s, rest = source[r], int(i < 3)
        if (r, rest) not in seen:
            seen.add((r, rest))
            chunks = pl.ds(0, 3 if rest else 1)
            arrived(pbuf.at[s, chunks, 0] if r == 0 else pbuf.at[s, chunks], p_recv.at[r, rest])

    def finish(r):
        arrived(crecv.at[r, pl.ds(1, 2)], c_recv.at[r, 2])
        pre_arrived(r, 3)
        s = source[r]
        for k in (0, 1):
            total = keep_own[r, k] + crecv[r, 2, k].astype(f32) + crecv[r, 1, 1 - k].astype(f32)
            dsend[r, k] = (total * gelu_slope(pbuf[s, col, k].astype(f32))).astype(bf16)
        mine = go.at[col, :, hidden(dep)]
        if r == 0:
            send(SHARE, dsend.at[0, other], mine, d_recv.at[0], at_depth(2 * x + other))
            local.append(pltpu.make_async_copy(dsend.at[0, core], mine, out_sem.at[0]))
            local[-1].start()
        else:
            for k in (0, 1):
                send(SHARE, dsend.at[r, k], mine, d_recv.at[4 - r], at_depth(2 * s + k))

    def piece(c, j):
        return go.at[c, :, hidden(j)]

    def e_own(r):
        s = source[r]
        if r == 0:
            arrived(piece(col, 2 * x + other), d_recv.at[0])
            local.pop(0).wait()
        else:
            arrived(dsend.at[r], d_recv.at[r])
        for flip in (0, 1):
            for k in (0, 1):
                part = piece(col, 2 * s + k)
                send(SPREAD, part, part, e_recv.at[r, 2 if flip else k], at_col((up, down)[k ^ flip]))

    def e_forward(r):
        for k, (frm, to) in enumerate(((down, up), (up, down))):
            part = piece(frm, 2 * source[r] + k)
            arrived(part, e_recv.at[r, k])
            send(SPREAD, part, part, e_recv.at[r, 2], at_col(to))

    def e_rest(r):
        arrived(crecv.at[r, pl.ds(0, 2)], e_recv.at[r, 2])

    def activate(r, i):
        pre_arrived(r, i)
        s, q = source[r], order[i]
        pre = pbuf[s, q].reshape(2 * chunk, wide).astype(f32)
        place = pl.ds(pl.multiple_of((4 * s + q) * 2 * chunk, 128), 2 * chunk)
        act_t[:, place] = gelu_value(pre).astype(bf16).T

    def weight_grad(r, n):
        s, cols = source[r], pl.ds(n * 512, 512)
        span = 8 * chunk
        part = jnp.dot(
            act_t[:, pl.ds(pl.multiple_of(s * span, 128), span)],
            gbuf[s, :, :, :, :, cols].reshape(span, 512),
            preferred_element_type=f32,
        )
        if r == 0:
            gw_sum[:, cols] = part
        elif r == 2:
            gw_buf[:, cols] = (gw_sum[:, cols] + part).astype(bf16)
            local.append(pltpu.make_async_copy(gw_buf.at[:, cols], gw.at[:, cols], out_sem.at[1 + n]))
            local[-1].start()
        else:
            gw_sum[:, cols] += part

    arrived(gbuf.at[x, :, other], s_recv)
    own_part(other)
    to_col(0, 0, other)
    to_col(0, 1, core)

    steps = dict(
        X=from_x, Y=from_y, G=group, C=combine, F=finish, O=e_own, W=e_forward, R=e_rest, A=activate, M=weight_grad,
        P=send_pre,
    )
    for name, *numbers in PLAN:
        steps[name](*numbers)
    every_grad = gbuf.reshape(64, part_rows, features)
    arrived(every_grad.at[pl.ds(0, 56)], sent.at[GRAD])
    arrived(pbuf.reshape(32, chunk, wide).at[pl.ds(0, 28)], sent.at[PRE])
    arrived(crecv, sent.at[SUM])
    arrived(dsend.reshape(8, chunk, wide).at[pl.ds(0, 7)], sent.at[SHARE])
    arrived(crecv, sent.at[SPREAD])
    for copy in local:
        copy.wait()


def write_results(go, gw, go_out, gw_out, sem):
    copies = []
    for n, (src, dst) in enumerate(((go, go_out), (gw, gw_out))):
        rows = src.shape[0] // 4
        for i in range(4):
            part = pl.ds(i * rows, rows)
            copies.append(pltpu.make_async_copy(src.at[part], dst.at[part], sem.at[n, i]))
    for copy in copies:
        copy.start()
    for copy in copies:
        copy.wait()


def on_device(grad_out, pre_act, down_weight):
    tokens, features = grad_out.shape
    hidden = pre_act.shape[1]
    wide = down_weight.shape[0]
    chunk = tokens // 4
    any_spec = pl.BlockSpec(memory_space=pl.ANY)
    dma = pltpu.SemaphoreType.DMA
    operands = (grad_out.reshape(4, 2, chunk // 2, features), pre_act.reshape(4, chunk, hidden), down_weight)
    grad_pre, grad_weight = pl.pallas_call(
        kernel,
        out_shape=(
            jax.ShapeDtypeStruct((4, chunk, hidden), bf16),
            jax.ShapeDtypeStruct((wide, features), bf16),
        ),
        in_specs=[any_spec] * 3,
        out_specs=(any_spec, any_spec),
        scratch_shapes=[
            pltpu.VMEM((4, 4, 2, 2, chunk // 2, features), bf16),
            pltpu.VMEM((4, 4, 2, chunk, wide), bf16),
            pltpu.VMEM((wide, features), bf16),
            pltpu.VMEM((2, 4, chunk, wide), f32),
            pltpu.VMEM((4, 3, 2, chunk, wide), bf16),
            pltpu.VMEM((4, 3, 2, chunk, wide), bf16),
            pltpu.VMEM((4, 2, chunk, wide), f32),
            pltpu.VMEM((4, 2, chunk, wide), f32),
            pltpu.VMEM((4, 2, chunk, wide), bf16),
            pltpu.VMEM((wide, 32 * chunk), bf16),
            pltpu.VMEM((wide, features), f32),
            pltpu.VMEM((wide, features), bf16),
            dma((3,)), dma((4,)), dma(()), dma((3, 4, 3)), dma((4, 2)), dma((4, 3)), dma((4,)), dma((4, 3)), dma((5,)),
        ],
        compiler_params=pltpu.CompilerParams(
            collective_id=0, has_side_effects=True, vmem_limit_bytes=44 * 1024 * 1024
        ),
    )(*(pltpu.with_memory_space_constraint(operand, pltpu.HBM) for operand in operands))
    return pl.pallas_call(
        write_results,
        out_shape=(
            jax.ShapeDtypeStruct((tokens, hidden), bf16),
            jax.ShapeDtypeStruct((wide, features), bf16),
        ),
        in_specs=[any_spec] * 2,
        out_specs=(any_spec, any_spec),
        scratch_shapes=[dma((2, 4))],
        compiler_params=pltpu.CompilerParams(vmem_limit_bytes=1024 * 1024),
    )(grad_pre.reshape(tokens, hidden), grad_weight)


def solution(mesh):
    placed = (P("depth", "col"), P("depth", "row"), P(("row", "depth"), "col"))
    return jax.shard_map(
        on_device,
        mesh=mesh,
        in_specs=placed,
        out_specs=(P("depth", "row"), P(("row", "depth"), "col")),
        check_vma=False,
    )
```

```python
import jax
import jax.numpy as jnp
from jax import lax
from jax.experimental import pallas as pl
from jax.experimental.pallas import tpu as pltpu
from jax.sharding import PartitionSpec as P

sqrt_two_pi = 0.7978845608028654
cubic_coeff = 0.044715
MESH = pl.DeviceIdType.MESH
bf16, f32 = jnp.bfloat16, jnp.float32


def gelu_value(preact):
    tangent = jnp.tanh(sqrt_two_pi * (preact + cubic_coeff * preact * preact * preact))
    return 0.5 * preact * (1.0 + tangent)


def gelu_slope(preact):
    tangent = jnp.tanh(sqrt_two_pi * (preact + cubic_coeff * preact * preact * preact))
    inner = sqrt_two_pi * (1.0 + 3.0 * cubic_coeff * preact * preact)
    return 0.5 * (1.0 + tangent) + 0.5 * preact * (1.0 - tangent * tangent) * inner


PLAN = [
    ("P", 3, 3), ("X", 3, 0), ("X", 1, 0), ("C", 0, 0), ("G", 1, 0), ("X", 1, 4), ("X", 3, 4), ("C", 0, 1), ("G",
    3, 4), ("G", 3, 0), ("X", 3, 1), ("X", 1, 2), ("G", 1, 4), ("A", 0, 3), ("G", 3, 1), ("G", 1, 2), ("A", 0, 0),
    ("F", 0), ("X", 3, 2), ("O", 0), ("X", 1, 1), ("G", 1, 1), ("X", 3, 3), ("C", 1, 1), ("X", 1, 3), ("G", 3, 2),
    ("C", 1, 0), ("X", 2, 0), ("G", 1, 3), ("G", 3, 3), ("P", 3, 1), ("X", 2, 4), ("G", 2, 0), ("G", 2, 4), ("C",
    3, 1), ("C", 3, 0), ("P", 0, 3), ("X", 2, 1), ("W", 0), ("X", 2, 2), ("F", 1), ("P", 3, 2), ("P", 0, 1), ("G",
    2, 1), ("G", 2, 2), ("X", 2, 3), ("P", 1, 1), ("C", 2, 1), ("A", 0, 1), ("C", 2, 0), ("A", 0, 2), ("F", 3),
    ("P", 2, 3), ("O", 3), ("P", 1, 3), ("M", 0, 2), ("A", 3, 3), ("G", 2, 3), ("M", 0, 0), ("O", 1), ("F", 2),
    ("P", 1, 2), ("W", 3), ("P", 2, 1), ("O", 2), ("P", 2, 2), ("P", 0, 2), ("W", 1), ("A", 1, 0), ("R", 0), ("A",
    1, 2), ("A", 2, 3), ("W", 2), ("A", 1, 3), ("A", 3, 1), ("A", 3, 0), ("A", 3, 2), ("M", 0, 1), ("M", 3, 1),
    ("A", 2, 1), ("M", 3, 0), ("A", 1, 1), ("M", 3, 2), ("A", 2, 2), ("M", 1, 0), ("A", 2, 0), ("R", 3), ("M", 1,
    2), ("M", 1, 1), ("M", 2, 1), ("M", 2, 0), ("M", 2, 2), ("R", 1), ("R", 2),
]


def kernel(
    g_hbm, p_hbm, w_hbm, go, gw,
    gbuf, pbuf, wbuf, first, csend, crecv, keep, keep_own, dsend, act_t, gw_sum, gw_buf,
    load_sem, out_sem, s_recv, a_recv, p_recv, c_recv, d_recv, e_recv, sent,
):
    row, col, dep = lax.axis_index("row"), lax.axis_index("col"), lax.axis_index("depth")
    x, core = dep // 2, dep % 2
    other = 1 - core
    part_rows, features = g_hbm.shape[2:]
    chunk = 2 * part_rows
    wide = wbuf.shape[0]
    right, left, far = (x + 1) % 4, (x + 3) % 4, (x + 2) % 4
    up, down = (col + 1) % 4, (col + 3) % 4
    order = [(col + 2) % 4, up, down, col]
    source = {0: x, 1: right, 2: far, 3: left}
    local = []

    def at_depth(d):
        return (row, col, d)

    def at_col(c):
        return (row, c, dep)

    GRAD, PRE, SUM, SHARE, SPREAD = range(5)

    def send(kind, src, dst, recv_sem, device):
        pltpu.make_async_remote_copy(
            src_ref=src, dst_ref=dst, send_sem=sent.at[kind], recv_sem=recv_sem, device_id=device, device_id_type=MESH
        ).start()

    def arrived(dst, recv_sem):
        pltpu.make_async_copy(dst, dst, recv_sem).wait()

    def hidden(d):
        return pl.ds(pl.multiple_of(d * wide, 128), wide)

    def times_weight(rows):
        return lax.dot_general(rows, wbuf[...], (((1,), (1,)), ((), ())), preferred_element_type=f32)

    barrier = pltpu.get_barrier_semaphore()
    for c in (up, down):
        pl.semaphore_signal(barrier, inc=1, device_id=at_col(c), device_id_type=MESH)
    for t in range(1, 8):
        pl.semaphore_signal(barrier, inc=1, device_id=at_depth((dep + t) % 8), device_id_type=MESH)
    loads = [
        pltpu.make_async_copy(w_hbm, wbuf, load_sem.at[0]),
        pltpu.make_async_copy(g_hbm, gbuf.at[x, :, core], load_sem.at[1]),
        pltpu.make_async_copy(p_hbm.at[:, :, hidden(dep)], pbuf.at[x, :, core], load_sem.at[2]),
    ]
    for copy in loads:
        copy.start()
    loads[0].wait()
    loads[1].wait()

    def own_part(k):
        rows = gbuf[x, :, k].reshape(4 * chunk, features)
        first[k] = times_weight(rows).reshape(4, chunk, wide)
        csend[0, 0, k] = first[k, order[0]].astype(bf16)
        csend[0, 1, 1 - k] = first[k, (col + 3 + 2 * k) % 4].astype(bf16)
        keep[0, k] = first[k, (col + 1 + 2 * k) % 4]
        keep_own[0, k] = first[k, col]

    own_part(core)
    loads[2].wait()
    pl.semaphore_wait(barrier, 9)

    def to_col(r, kind, way, rows=slice(None)):
        sem = c_recv.at[r, way] if kind == 0 else c_recv.at[r, 2]
        src, dst = csend.at[r, kind, way, rows], crecv.at[r, kind, way, rows]
        send(SUM, src, dst, sem, at_col((col + 1 + 2 * way) % 4))

    def token_rows(s, i, c):
        if i % 4:
            return gbuf.at[s, order[i], c]
        return gbuf.at[s, order[0], c, i // 4]

    def send_grad(i, r, d):
        mine = token_rows(x, i, core)
        send(GRAD, mine, mine, a_recv.at[r - 1, i, 0], at_depth(d))

    def send_pre(i, t):
        q = order[i]
        sem = p_recv.at[(4 - t) % 4, 0 if i == 3 else 1]
        for d in (2 * ((x + t) % 4) + core, 2 * ((x + t) % 4) + other)[0 if t else 1 :]:
            send(PRE, p_hbm.at[q, :, hidden(d)], pbuf.at[x, q, core], sem, at_depth(d))

    send_grad(0, 3, 2 * right + core)
    send_grad(0, 1, 2 * left + core)
    to_col(0, 0, core)
    to_col(0, 1, other)
    mine = gbuf.at[x, :, core]
    send(GRAD, mine, mine, s_recv, at_depth(2 * x + other))
    for i, j in ((4, 4), (1, 2), (2, 1), (3, 3)):
        send_grad(i, 3, 2 * right + core)
        send_grad(j, 1, 2 * left + core)
    for i in (3, 0, 1, 2):
        send_pre(i, 0)

    def from_x(r, i):
        part, sem = token_rows(source[r], i, core), a_recv.at[r - 1, i]
        arrived(part, sem.at[0])
        send(GRAD, part, part, sem.at[1], at_depth(2 * x + other))
        if r == 3 and i in (0, 4, 1):
            send(GRAD, part, part, a_recv.at[1, i, 0], at_depth(2 * right + core))
        if r == 1 and i in (2, 3):
            send(GRAD, part, part, a_recv.at[1, i, 0], at_depth(2 * left + core))

    def group(r, i):
        s = source[r]
        arrived(token_rows(s, i, other), a_recv.at[r - 1, i, 1])
        if i % 4 == 0:
            h = i // 4
            part = times_weight(gbuf[s, order[0], :, h].reshape(chunk, features)).astype(bf16)
            rows = pl.ds(h * part_rows, part_rows)
            for way in (0, 1):
                csend[r, 0, way, rows] = part[way * part_rows : (way + 1) * part_rows]
                to_col(r, 0, way, rows)
            return
        part = times_weight(gbuf[s, order[i]].reshape(2 * chunk, features))
        low, high = part[:chunk], part[chunk:]
        if i == 1:
            csend[r, 1, 0] = high.astype(bf16)
            keep[r, 0] = low
            to_col(r, 1, 0)
        elif i == 2:
            csend[r, 1, 1] = low.astype(bf16)
            keep[r, 1] = high
            to_col(r, 1, 1)
        else:
            keep_own[r, 0] = low
            keep_own[r, 1] = high

    def combine(r, way):
        if r == 0:
            way = (core, other)[way]
        arrived(crecv.at[r, 0, way], c_recv.at[r, way])
        csend[r, 2, way] = (keep[r, way] + crecv[r, 0, way].astype(f32)).astype(bf16)
        to_col(r, 2, way)

    seen = set()

    def pre_arrived(r, i):
        s, rest = source[r], int(i < 3)
        if (r, rest) not in seen:
            seen.add((r, rest))
            chunks = pl.ds(0, 3 if rest else 1)
            arrived(pbuf.at[s, chunks, 0] if r == 0 else pbuf.at[s, chunks], p_recv.at[r, rest])

    def finish(r):
        arrived(crecv.at[r, pl.ds(1, 2)], c_recv.at[r, 2])
        pre_arrived(r, 3)
        s = source[r]
        for k in (0, 1):
            total = keep_own[r, k] + crecv[r, 2, k].astype(f32) + crecv[r, 1, 1 - k].astype(f32)
            dsend[r, k] = (total * gelu_slope(pbuf[s, col, k].astype(f32))).astype(bf16)
        mine = go.at[col, :, hidden(dep)]
        if r == 0:
            send(SHARE, dsend.at[0, other], mine, d_recv.at[0], at_depth(2 * x + other))
            local.append(pltpu.make_async_copy(dsend.at[0, core], mine, out_sem.at[0]))
            local[-1].start()
        else:
            for k in (0, 1):
                send(SHARE, dsend.at[r, k], mine, d_recv.at[4 - r], at_depth(2 * s + k))

    def piece(c, j):
        return go.at[c, :, hidden(j)]

    def e_own(r):
        s = source[r]
        if r == 0:
            arrived(piece(col, 2 * x + other), d_recv.at[0])
            local.pop(0).wait()
        else:
            arrived(dsend.at[r], d_recv.at[r])
        for flip in (0, 1):
            for k in (0, 1):
                part = piece(col, 2 * s + k)
                send(SPREAD, part, part, e_recv.at[r, 2 if flip else k], at_col((up, down)[k ^ flip]))

    def e_forward(r):
        for k, (frm, to) in enumerate(((down, up), (up, down))):
            part = piece(frm, 2 * source[r] + k)
            arrived(part, e_recv.at[r, k])
            send(SPREAD, part, part, e_recv.at[r, 2], at_col(to))

    def e_rest(r):
        arrived(crecv.at[r, pl.ds(0, 2)], e_recv.at[r, 2])

    def activate(r, i):
        pre_arrived(r, i)
        s, q = source[r], order[i]
        pre = pbuf[s, q].reshape(2 * chunk, wide).astype(f32)
        place = pl.ds(pl.multiple_of((4 * s + q) * 2 * chunk, 128), 2 * chunk)
        act_t[:, place] = gelu_value(pre).astype(bf16).T

    def weight_grad(r, n):
        s, cols = source[r], pl.ds(n * 512, 512)
        span = 8 * chunk
        part = jnp.dot(
            act_t[:, pl.ds(pl.multiple_of(s * span, 128), span)],
            gbuf[s, :, :, :, :, cols].reshape(span, 512),
            preferred_element_type=f32,
        )
        if r == 0:
            gw_sum[:, cols] = part
        elif r == 2:
            gw_buf[:, cols] = (gw_sum[:, cols] + part).astype(bf16)
            local.append(pltpu.make_async_copy(gw_buf.at[:, cols], gw.at[:, cols], out_sem.at[1 + n]))
            local[-1].start()
        else:
            gw_sum[:, cols] += part

    arrived(gbuf.at[x, :, other], s_recv)
    own_part(other)
    to_col(0, 0, other)
    to_col(0, 1, core)

    steps = dict(
        X=from_x, G=group, C=combine, F=finish, O=e_own, W=e_forward, R=e_rest, A=activate, M=weight_grad,
        P=send_pre,
    )
    for name, *numbers in PLAN:
        steps[name](*numbers)
    every_grad = gbuf.reshape(64, part_rows, features)
    arrived(every_grad.at[pl.ds(0, 56)], sent.at[GRAD])
    arrived(pbuf.reshape(32, chunk, wide).at[pl.ds(0, 28)], sent.at[PRE])
    arrived(crecv, sent.at[SUM])
    arrived(dsend.reshape(8, chunk, wide).at[pl.ds(0, 7)], sent.at[SHARE])
    arrived(crecv, sent.at[SPREAD])
    for copy in local:
        copy.wait()


def write_results(go, gw, go_out, gw_out, sem):
    copies = []
    for n, (src, dst) in enumerate(((go, go_out), (gw, gw_out))):
        rows = src.shape[0] // 4
        for i in range(4):
            part = pl.ds(i * rows, rows)
            copies.append(pltpu.make_async_copy(src.at[part], dst.at[part], sem.at[n, i]))
    for copy in copies:
        copy.start()
    for copy in copies:
        copy.wait()


def on_device(grad_out, pre_act, down_weight):
    tokens, features = grad_out.shape
    hidden = pre_act.shape[1]
    wide = down_weight.shape[0]
    chunk = tokens // 4
    any_spec = pl.BlockSpec(memory_space=pl.ANY)
    dma = pltpu.SemaphoreType.DMA
    operands = (grad_out.reshape(4, 2, chunk // 2, features), pre_act.reshape(4, chunk, hidden), down_weight)
    grad_pre, grad_weight = pl.pallas_call(
        kernel,
        out_shape=(
            jax.ShapeDtypeStruct((4, chunk, hidden), bf16),
            jax.ShapeDtypeStruct((wide, features), bf16),
        ),
        in_specs=[any_spec] * 3,
        out_specs=(any_spec, any_spec),
        scratch_shapes=[
            pltpu.VMEM((4, 4, 2, 2, chunk // 2, features), bf16),
            pltpu.VMEM((4, 4, 2, chunk, wide), bf16),
            pltpu.VMEM((wide, features), bf16),
            pltpu.VMEM((2, 4, chunk, wide), f32),
            pltpu.VMEM((4, 3, 2, chunk, wide), bf16),
            pltpu.VMEM((4, 3, 2, chunk, wide), bf16),
            pltpu.VMEM((4, 2, chunk, wide), f32),
            pltpu.VMEM((4, 2, chunk, wide), f32),
            pltpu.VMEM((4, 2, chunk, wide), bf16),
            pltpu.VMEM((wide, 32 * chunk), bf16),
            pltpu.VMEM((wide, features), f32),
            pltpu.VMEM((wide, features), bf16),
            dma((3,)), dma((4,)), dma(()), dma((3, 5, 2)), dma((4, 2)), dma((4, 3)), dma((4,)), dma((4, 3)), dma((5,)),
        ],
        compiler_params=pltpu.CompilerParams(
            collective_id=0, has_side_effects=True, vmem_limit_bytes=44 * 1024 * 1024
        ),
    )(*(pltpu.with_memory_space_constraint(operand, pltpu.HBM) for operand in operands))
    return pl.pallas_call(
        write_results,
        out_shape=(
            jax.ShapeDtypeStruct((tokens, hidden), bf16),
            jax.ShapeDtypeStruct((wide, features), bf16),
        ),
        in_specs=[any_spec] * 2,
        out_specs=(any_spec, any_spec),
        scratch_shapes=[dma((2, 4))],
        compiler_params=pltpu.CompilerParams(vmem_limit_bytes=1024 * 1024),
    )(grad_pre.reshape(tokens, hidden), grad_weight)


def solution(mesh):
    placed = (P("depth", "col"), P("depth", "row"), P(("row", "depth"), "col"))
    return jax.shard_map(
        on_device,
        mesh=mesh,
        in_specs=placed,
        out_specs=(P("depth", "row"), P(("row", "depth"), "col")),
        check_vma=False,
    )
```

```python
import jax
import jax.numpy as jnp
from jax import lax
from jax.experimental import pallas as pl
from jax.experimental.pallas import tpu as pltpu
from jax.sharding import PartitionSpec as P

sqrt_two_pi = 0.7978845608028654
cubic_coeff = 0.044715
MESH = pl.DeviceIdType.MESH
bf16, f32 = jnp.bfloat16, jnp.float32


def gelu_value(preact):
    tangent = jnp.tanh(sqrt_two_pi * (preact + cubic_coeff * preact * preact * preact))
    return 0.5 * preact * (1.0 + tangent)


def gelu_slope(preact):
    tangent = jnp.tanh(sqrt_two_pi * (preact + cubic_coeff * preact * preact * preact))
    inner = sqrt_two_pi * (1.0 + 3.0 * cubic_coeff * preact * preact)
    return 0.5 * (1.0 + tangent) + 0.5 * preact * (1.0 - tangent * tangent) * inner


SPLIT = (0,)

PLAN = [
    ("X", 1, 0), ("X", 3, 0), ("G", 3, 0), ("C", 0, 0), ("C", 0, 1), ("A", 0, 3), ("X", 3, 4), ("G", 1, 0), ("X",
    1, 4), ("G", 3, 4), ("X", 1, 2), ("G", 1, 4), ("X", 3, 1), ("G", 1, 2), ("G", 3, 1), ("F", 0), ("O", 0), ("P",
    3, 3), ("X", 1, 1), ("G", 1, 1), ("C", 1, 1), ("A", 0, 1), ("X", 3, 2), ("X", 1, 3), ("P", 3, 1), ("G", 3, 2),
    ("X", 3, 3), ("C", 1, 0), ("P", 0, 3), ("C", 3, 0), ("C", 3, 1), ("A", 0, 2), ("G", 1, 3), ("A", 0, 0), ("X",
    2, 4), ("X", 2, 0), ("G", 2, 0), ("G", 2, 4), ("X", 2, 2), ("P", 2, 3), ("W", 0), ("X", 2, 1), ("F", 1), ("G",
    2, 2), ("P", 3, 2), ("M", 0, 1), ("G", 2, 1), ("G", 3, 3), ("F", 3), ("C", 2, 1), ("P", 1, 3), ("P", 2, 1),
    ("X", 2, 3), ("C", 2, 0), ("P", 1, 1), ("P", 0, 1), ("G", 2, 3), ("O", 3), ("M", 0, 0), ("F", 2), ("O", 1),
    ("A", 1, 2), ("A", 1, 0), ("W", 3), ("M", 0, 2), ("A", 3, 3), ("A", 1, 1), ("P", 2, 2), ("A", 3, 1), ("O", 2),
    ("A", 2, 3), ("P", 0, 2), ("A", 3, 0), ("W", 1), ("A", 1, 3), ("P", 1, 2), ("W", 2), ("R", 3), ("M", 1, 1),
    ("A", 3, 2), ("A", 2, 2), ("M", 3, 0), ("A", 2, 0), ("M", 1, 2), ("M", 1, 0), ("A", 2, 1), ("M", 2, 0), ("M",
    3, 2), ("M", 2, 2), ("M", 3, 1), ("M", 2, 1), ("R", 2), ("R", 0), ("R", 1),
]


def kernel(
    g_hbm, p_hbm, w_hbm, go, gw,
    gbuf, pbuf, wbuf, first, csend, crecv, keep, keep_own, dsend, act_t, gw_sum, gw_buf,
    load_sem, out_sem, s_recv, a_recv, p_recv, c_recv, d_recv, e_recv, sent,
):
    row, col, dep = lax.axis_index("row"), lax.axis_index("col"), lax.axis_index("depth")
    x, core = dep // 2, dep % 2
    other = 1 - core
    part_rows, features = g_hbm.shape[2:]
    chunk = 2 * part_rows
    wide = wbuf.shape[0]
    right, left, far = (x + 1) % 4, (x + 3) % 4, (x + 2) % 4
    up, down = (col + 1) % 4, (col + 3) % 4
    order = [(col + 2) % 4, up, down, col]
    source = {0: x, 1: right, 2: far, 3: left}
    local = []

    def at_depth(d):
        return (row, col, d)

    def at_col(c):
        return (row, c, dep)

    GRAD, PRE, SUM, SHARE, SPREAD = range(5)

    def send(kind, src, dst, recv_sem, device):
        pltpu.make_async_remote_copy(
            src_ref=src, dst_ref=dst, send_sem=sent.at[kind], recv_sem=recv_sem, device_id=device, device_id_type=MESH
        ).start()

    def arrived(dst, recv_sem):
        pltpu.make_async_copy(dst, dst, recv_sem).wait()

    def hidden(d):
        return pl.ds(pl.multiple_of(d * wide, 128), wide)

    def times_weight(rows):
        return lax.dot_general(rows, wbuf[...], (((1,), (1,)), ((), ())), preferred_element_type=f32)

    barrier = pltpu.get_barrier_semaphore()
    for c in (up, down):
        pl.semaphore_signal(barrier, inc=1, device_id=at_col(c), device_id_type=MESH)
    for t in range(1, 8):
        pl.semaphore_signal(barrier, inc=1, device_id=at_depth((dep + t) % 8), device_id_type=MESH)
    loads = [
        pltpu.make_async_copy(w_hbm, wbuf, load_sem.at[0]),
        pltpu.make_async_copy(g_hbm, gbuf.at[x, :, core], load_sem.at[1]),
        pltpu.make_async_copy(p_hbm.at[:, :, hidden(dep)], pbuf.at[x, :, core], load_sem.at[2]),
    ]
    for copy in loads:
        copy.start()
    loads[0].wait()
    loads[1].wait()

    def own_part(k):
        rows = gbuf[x, :, k].reshape(4 * chunk, features)
        first[k] = times_weight(rows).reshape(4, chunk, wide)
        csend[0, 1, 1 - k] = first[k, (col + 3 + 2 * k) % 4].astype(bf16)
        keep[0, k] = first[k, (col + 1 + 2 * k) % 4]
        keep_own[0, k] = first[k, col]

    def far_part(k):
        csend[0, 0, k] = times_weight(gbuf[x, order[0], k].reshape(chunk, features)).astype(bf16)

    own_part(core)
    csend[0, 0, core] = first[core, order[0]].astype(bf16)
    loads[2].wait()
    pl.semaphore_wait(barrier, 9)

    def to_col(r, kind, way, rows=slice(None)):
        sem = c_recv.at[r, way] if kind == 0 else c_recv.at[r, 2]
        src, dst = csend.at[r, kind, way, rows], crecv.at[r, kind, way, rows]
        send(SUM, src, dst, sem, at_col((col + 1 + 2 * way) % 4))

    def token_rows(s, i, c):
        whole = gbuf.at[s, order[i % 4], c]
        return whole.at[i // 4] if i % 4 in SPLIT else whole

    def send_grad(i, r, d):
        mine = token_rows(x, i, core)
        send(GRAD, mine, mine, a_recv.at[r - 1, i, 0], at_depth(d))

    def send_pre(i, t):
        q = order[i]
        sem = p_recv.at[(4 - t) % 4, 0 if i == 3 else 1]
        for d in (2 * ((x + t) % 4) + core, 2 * ((x + t) % 4) + other)[0 if t else 1 :]:
            send(PRE, p_hbm.at[q, :, hidden(d)], pbuf.at[x, q, core], sem, at_depth(d))

    send_grad(0, 3, 2 * right + core)
    send_grad(0, 1, 2 * left + core)
    to_col(0, 0, core)
    to_col(0, 1, other)
    for i, q in enumerate(order):
        mine = gbuf.at[x, q, core]
        send(GRAD, mine, mine, s_recv.at[min(i, 1)], at_depth(2 * x + other))
    for i, j in ((0, 0), (1, 2), (2, 1), (3, 3)):
        for h in (0, 1):
            if h == 1 and i in SPLIT or h == 0 and i != 0:
                send_grad(i + 4 * h, 3, 2 * right + core)
            if h == 1 and j in SPLIT or h == 0 and j != 0:
                send_grad(j + 4 * h, 1, 2 * left + core)
    for i in (3, 0, 1, 2):
        send_pre(i, 0)

    def from_x(r, i):
        part, sem = token_rows(source[r], i, core), a_recv.at[r - 1, i]
        arrived(part, sem.at[0])
        send(GRAD, part, part, sem.at[1], at_depth(2 * x + other))
        if r == 3 and i % 4 < 2:
            send(GRAD, part, part, a_recv.at[1, i, 0], at_depth(2 * right + core))
        if r == 1 and i % 4 >= 2:
            send(GRAD, part, part, a_recv.at[1, i, 0], at_depth(2 * left + core))

    def group(r, i):
        s = source[r]
        arrived(token_rows(s, i, other), a_recv.at[r - 1, i, 1])
        q, h, count, i = order[i % 4], i // 4, part_rows, i % 4
        if i in SPLIT:
            tokens = gbuf[s, q, :, h]
        else:
            tokens, count = gbuf[s, q], chunk
        part = times_weight(tokens.reshape(2 * count, features))
        low, high = part[:count], part[count:]
        rows = pl.ds(h * count, count)
        if i == 0:
            csend[r, 0, 0, rows] = low.astype(bf16)
            csend[r, 0, 1, rows] = high.astype(bf16)
            to_col(r, 0, 0, rows)
            to_col(r, 0, 1, rows)
        elif i == 1:
            csend[r, 1, 0, rows] = high.astype(bf16)
            keep[r, 0, rows] = low
            to_col(r, 1, 0, rows)
        elif i == 2:
            csend[r, 1, 1, rows] = low.astype(bf16)
            keep[r, 1, rows] = high
            to_col(r, 1, 1, rows)
        else:
            keep_own[r, 0, rows] = low
            keep_own[r, 1, rows] = high

    def combine(r, way):
        if r == 0:
            way = (core, other)[way]
        arrived(crecv.at[r, 0, way], c_recv.at[r, way])
        csend[r, 2, way] = (keep[r, way] + crecv[r, 0, way].astype(f32)).astype(bf16)
        to_col(r, 2, way)

    seen = set()

    def pre_arrived(r, i):
        s, rest = source[r], int(i < 3)
        if (r, rest) not in seen:
            seen.add((r, rest))
            chunks = pl.ds(0, 3 if rest else 1)
            arrived(pbuf.at[s, chunks, 0] if r == 0 else pbuf.at[s, chunks], p_recv.at[r, rest])

    def finish(r):
        arrived(crecv.at[r, pl.ds(1, 2)], c_recv.at[r, 2])
        pre_arrived(r, 3)
        s = source[r]
        for k in (0, 1):
            total = keep_own[r, k] + crecv[r, 2, k].astype(f32) + crecv[r, 1, 1 - k].astype(f32)
            dsend[r, k] = (total * gelu_slope(pbuf[s, col, k].astype(f32))).astype(bf16)
        mine = go.at[col, :, hidden(dep)]
        if r == 0:
            send(SHARE, dsend.at[0, other], mine, d_recv.at[0], at_depth(2 * x + other))
            local.append(pltpu.make_async_copy(dsend.at[0, core], mine, out_sem.at[0]))
            local[-1].start()
        else:
            for k in (0, 1):
                send(SHARE, dsend.at[r, k], mine, d_recv.at[4 - r], at_depth(2 * s + k))

    def piece(c, j):
        return go.at[c, :, hidden(j)]

    def e_own(r):
        s = source[r]
        if r == 0:
            arrived(piece(col, 2 * x + other), d_recv.at[0])
            local.pop(0).wait()
        else:
            arrived(dsend.at[r], d_recv.at[r])
        for flip in (0, 1):
            for k in (0, 1):
                part = piece(col, 2 * s + k)
                send(SPREAD, part, part, e_recv.at[r, 2 if flip else k], at_col((up, down)[k ^ flip]))

    def e_forward(r):
        for k, (frm, to) in enumerate(((down, up), (up, down))):
            part = piece(frm, 2 * source[r] + k)
            arrived(part, e_recv.at[r, k])
            send(SPREAD, part, part, e_recv.at[r, 2], at_col(to))

    def e_rest(r):
        arrived(crecv.at[r, pl.ds(0, 2)], e_recv.at[r, 2])

    def activate(r, i):
        pre_arrived(r, i)
        s, q = source[r], order[i]
        pre = pbuf[s, q].reshape(2 * chunk, wide).astype(f32)
        place = pl.ds(pl.multiple_of((4 * s + q) * 2 * chunk, 128), 2 * chunk)
        act_t[:, place] = gelu_value(pre).astype(bf16).T

    def weight_grad(r, n):
        s, cols = source[r], pl.ds(n * 512, 512)
        span = 8 * chunk
        part = jnp.dot(
            act_t[:, pl.ds(pl.multiple_of(s * span, 128), span)],
            gbuf[s, :, :, :, :, cols].reshape(span, 512),
            preferred_element_type=f32,
        )
        if r == 0:
            gw_sum[:, cols] = part
        elif r == 2:
            gw_buf[:, cols] = (gw_sum[:, cols] + part).astype(bf16)
            local.append(pltpu.make_async_copy(gw_buf.at[:, cols], gw.at[:, cols], out_sem.at[1 + n]))
            local[-1].start()
        else:
            gw_sum[:, cols] += part

    arrived(gbuf.at[x, order[0], other], s_recv.at[0])
    far_part(other)
    to_col(0, 0, other)
    arrived(gbuf.at[x, pl.ds(0, 3), other], s_recv.at[1])
    own_part(other)
    to_col(0, 1, core)

    steps = dict(
        X=from_x, G=group, C=combine, F=finish, O=e_own, W=e_forward, R=e_rest, A=activate, M=weight_grad,
        P=send_pre,
    )
    for name, *numbers in PLAN:
        steps[name](*numbers)
    every_grad = gbuf.reshape(64, part_rows, features)
    arrived(every_grad.at[pl.ds(0, 56)], sent.at[GRAD])
    arrived(pbuf.reshape(32, chunk, wide).at[pl.ds(0, 28)], sent.at[PRE])
    arrived(crecv, sent.at[SUM])
    arrived(dsend.reshape(8, chunk, wide).at[pl.ds(0, 7)], sent.at[SHARE])
    arrived(crecv, sent.at[SPREAD])
    for copy in local:
        copy.wait()


def write_results(go, gw, go_out, gw_out, sem):
    copies = []
    for n, (src, dst) in enumerate(((go, go_out), (gw, gw_out))):
        rows = src.shape[0] // 2
        for i in range(2):
            part = pl.ds(i * rows, rows)
            copies.append(pltpu.make_async_copy(src.at[part], dst.at[part], sem.at[n, i]))
    for copy in copies:
        copy.start()
    for copy in copies:
        copy.wait()


def on_device(grad_out, pre_act, down_weight):
    tokens, features = grad_out.shape
    hidden = pre_act.shape[1]
    wide = down_weight.shape[0]
    chunk = tokens // 4
    any_spec = pl.BlockSpec(memory_space=pl.ANY)
    dma = pltpu.SemaphoreType.DMA
    operands = (grad_out.reshape(4, 2, chunk // 2, features), pre_act.reshape(4, chunk, hidden), down_weight)
    grad_pre, grad_weight = pl.pallas_call(
        kernel,
        out_shape=(
            jax.ShapeDtypeStruct((4, chunk, hidden), bf16),
            jax.ShapeDtypeStruct((wide, features), bf16),
        ),
        in_specs=[any_spec] * 3,
        out_specs=(any_spec, any_spec),
        scratch_shapes=[
            pltpu.VMEM((4, 4, 2, 2, chunk // 2, features), bf16),
            pltpu.VMEM((4, 4, 2, chunk, wide), bf16),
            pltpu.VMEM((wide, features), bf16),
            pltpu.VMEM((2, 4, chunk, wide), f32),
            pltpu.VMEM((4, 3, 2, chunk, wide), bf16),
            pltpu.VMEM((4, 3, 2, chunk, wide), bf16),
            pltpu.VMEM((4, 2, chunk, wide), f32),
            pltpu.VMEM((4, 2, chunk, wide), f32),
            pltpu.VMEM((4, 2, chunk, wide), bf16),
            pltpu.VMEM((wide, 32 * chunk), bf16),
            pltpu.VMEM((wide, features), f32),
            pltpu.VMEM((wide, features), bf16),
            dma((3,)), dma((4,)), dma((2,)), dma((3, 5, 2)), dma((4, 2)), dma((4, 3)), dma((4,)), dma((4, 3)), dma((5,)),
        ],
        compiler_params=pltpu.CompilerParams(
            collective_id=0, has_side_effects=True, vmem_limit_bytes=44 * 1024 * 1024
        ),
    )(*(pltpu.with_memory_space_constraint(operand, pltpu.HBM) for operand in operands))
    return pl.pallas_call(
        write_results,
        out_shape=(
            jax.ShapeDtypeStruct((tokens, hidden), bf16),
            jax.ShapeDtypeStruct((wide, features), bf16),
        ),
        in_specs=[any_spec] * 2,
        out_specs=(any_spec, any_spec),
        scratch_shapes=[dma((2, 2))],
        compiler_params=pltpu.CompilerParams(vmem_limit_bytes=1024 * 1024),
    )(grad_pre.reshape(tokens, hidden), grad_weight)


def solution(mesh):
    placed = (P("depth", "col"), P("depth", "row"), P(("row", "depth"), "col"))
    return jax.shard_map(
        on_device,
        mesh=mesh,
        in_specs=placed,
        out_specs=(P("depth", "row"), P(("row", "depth"), "col")),
        check_vma=False,
    )
```

```python
import jax
import jax.numpy as jnp
from jax import lax
from jax.experimental import pallas as pl
from jax.experimental.pallas import tpu as pltpu
from jax.sharding import PartitionSpec as P

sqrt_two_pi = 0.7978845608028654
cubic_coeff = 0.044715
MESH = pl.DeviceIdType.MESH
bf16, f32 = jnp.bfloat16, jnp.float32


def gelu_value(preact):
    tangent = jnp.tanh(sqrt_two_pi * (preact + cubic_coeff * preact * preact * preact))
    return 0.5 * preact * (1.0 + tangent)


def gelu_slope(preact):
    tangent = jnp.tanh(sqrt_two_pi * (preact + cubic_coeff * preact * preact * preact))
    inner = sqrt_two_pi * (1.0 + 3.0 * cubic_coeff * preact * preact)
    return 0.5 * (1.0 + tangent) + 0.5 * preact * (1.0 - tangent * tangent) * inner


SPLIT = (0,)

PLAN = [
    ("X", 1, 0), ("X", 3, 0), ("G", 3, 0), ("C", 0, 0), ("C", 0, 1), ("A", 0, 3), ("X", 3, 4), ("G", 1, 0), ("X",
    1, 4), ("G", 3, 4), ("X", 1, 2), ("G", 1, 4), ("X", 3, 1), ("G", 1, 2), ("G", 3, 1), ("P", 3, 3), ("F", 0),
    ("O", 0), ("X", 1, 1), ("G", 1, 1), ("C", 1, 1), ("A", 0, 1), ("X", 3, 2), ("X", 1, 3), ("P", 3, 1), ("G", 3,
    2), ("C", 1, 0), ("X", 3, 3), ("P", 0, 3), ("C", 3, 0), ("C", 3, 1), ("A", 0, 2), ("G", 1, 3), ("A", 0, 0),
    ("X", 2, 4), ("X", 2, 0), ("G", 2, 0), ("G", 2, 4), ("X", 2, 2), ("P", 2, 3), ("W", 0), ("X", 2, 1), ("F", 1),
    ("G", 2, 2), ("P", 3, 2), ("M", 0, 1), ("G", 2, 1), ("G", 3, 3), ("F", 3), ("C", 2, 1), ("P", 2, 1), ("X", 2,
    3), ("P", 1, 3), ("P", 1, 1), ("C", 2, 0), ("P", 0, 1), ("G", 2, 3), ("O", 3), ("F", 2), ("O", 1), ("A", 1,
    2), ("A", 1, 0), ("M", 0, 0), ("W", 3), ("M", 0, 2), ("A", 3, 3), ("A", 1, 1), ("P", 2, 2), ("A", 3, 1), ("O",
    2), ("A", 2, 3), ("P", 0, 2), ("A", 3, 0), ("A", 3, 2), ("W", 1), ("A", 1, 3), ("P", 1, 2), ("W", 2), ("R",
    3), ("M", 1, 1), ("A", 2, 2), ("M", 3, 0), ("A", 2, 0), ("M", 1, 2), ("M", 1, 0), ("M", 3, 2), ("A", 2, 1),
    ("M", 2, 0), ("M", 2, 2), ("M", 3, 1), ("M", 2, 1), ("R", 2), ("R", 0), ("R", 1),
]


def kernel(
    g_hbm, p_hbm, w_hbm, go, gw,
    gbuf, pbuf, wbuf, first, csend, crecv, keep, keep_own, dsend, act_t, gw_sum, gw_buf,
    load_sem, out_sem, s_recv, a_recv, p_recv, c_recv, d_recv, e_recv, sent,
):
    row, col, dep = lax.axis_index("row"), lax.axis_index("col"), lax.axis_index("depth")
    x, core = dep // 2, dep % 2
    other = 1 - core
    part_rows, features = g_hbm.shape[2:]
    chunk = 2 * part_rows
    wide = wbuf.shape[0]
    right, left, far = (x + 1) % 4, (x + 3) % 4, (x + 2) % 4
    up, down = (col + 1) % 4, (col + 3) % 4
    order = [(col + 2) % 4, up, down, col]
    source = {0: x, 1: right, 2: far, 3: left}
    local = []

    def at_depth(d):
        return (row, col, d)

    def at_col(c):
        return (row, c, dep)

    GRAD, PRE, SUM, SHARE, SPREAD = range(5)

    def send(kind, src, dst, recv_sem, device):
        pltpu.make_async_remote_copy(
            src_ref=src, dst_ref=dst, send_sem=sent.at[kind], recv_sem=recv_sem, device_id=device, device_id_type=MESH
        ).start()

    def arrived(dst, recv_sem):
        pltpu.make_async_copy(dst, dst, recv_sem).wait()

    def hidden(d):
        return pl.ds(pl.multiple_of(d * wide, 128), wide)

    def times_weight(rows):
        return lax.dot_general(rows, wbuf[...], (((1,), (1,)), ((), ())), preferred_element_type=f32)

    barrier = pltpu.get_barrier_semaphore()
    for c in (up, down):
        pl.semaphore_signal(barrier, inc=1, device_id=at_col(c), device_id_type=MESH)
    for t in range(1, 8):
        pl.semaphore_signal(barrier, inc=1, device_id=at_depth((dep + t) % 8), device_id_type=MESH)
    loads = [
        pltpu.make_async_copy(w_hbm, wbuf, load_sem.at[0]),
        pltpu.make_async_copy(g_hbm, gbuf.at[x, :, core], load_sem.at[1]),
        pltpu.make_async_copy(p_hbm.at[:, :, hidden(dep)], pbuf.at[x, :, core], load_sem.at[2]),
    ]
    for copy in loads:
        copy.start()
    loads[0].wait()
    loads[1].wait()

    def own_part(k):
        rows = gbuf[x, :, k].reshape(4 * chunk, features)
        first[k] = times_weight(rows).reshape(4, chunk, wide)
        csend[0, 1, 1 - k] = first[k, (col + 3 + 2 * k) % 4].astype(bf16)
        keep[0, k] = first[k, (col + 1 + 2 * k) % 4]
        keep_own[0, k] = first[k, col]

    def far_part(k):
        csend[0, 0, k] = times_weight(gbuf[x, order[0], k].reshape(chunk, features)).astype(bf16)

    own_part(core)
    csend[0, 0, core] = first[core, order[0]].astype(bf16)
    loads[2].wait()
    pl.semaphore_wait(barrier, 9)

    def to_col(r, kind, way, rows=slice(None)):
        sem = c_recv.at[r, way] if kind == 0 else c_recv.at[r, 2]
        src, dst = csend.at[r, kind, way, rows], crecv.at[r, kind, way, rows]
        send(SUM, src, dst, sem, at_col((col + 1 + 2 * way) % 4))

    def token_rows(s, i, c):
        whole = gbuf.at[s, order[i % 4], c]
        return whole.at[i // 4] if i % 4 in SPLIT else whole

    def send_grad(i, r, d):
        mine = token_rows(x, i, core)
        send(GRAD, mine, mine, a_recv.at[r - 1, i, 0], at_depth(d))

    def send_pre(i, t):
        q = order[i]
        sem = p_recv.at[(4 - t) % 4, 0 if i == 3 else 1]
        for d in (2 * ((x + t) % 4) + core, 2 * ((x + t) % 4) + other)[0 if t else 1 :]:
            send(PRE, p_hbm.at[q, :, hidden(d)], pbuf.at[x, q, core], sem, at_depth(d))

    send_grad(0, 3, 2 * right + core)
    send_grad(0, 1, 2 * left + core)
    to_col(0, 0, core)
    to_col(0, 1, other)
    for i, q in enumerate(order):
        mine = gbuf.at[x, q, core]
        send(GRAD, mine, mine, s_recv.at[min(i, 1)], at_depth(2 * x + other))
    for i, j in ((0, 0), (1, 2), (2, 1), (3, 3)):
        for h in (0, 1):
            if h == 1 and i in SPLIT or h == 0 and i != 0:
                send_grad(i + 4 * h, 3, 2 * right + core)
            if h == 1 and j in SPLIT or h == 0 and j != 0:
                send_grad(j + 4 * h, 1, 2 * left + core)
    for i in (3, 0, 1, 2):
        send_pre(i, 0)

    def from_x(r, i):
        part, sem = token_rows(source[r], i, core), a_recv.at[r - 1, i]
        arrived(part, sem.at[0])
        send(GRAD, part, part, sem.at[1], at_depth(2 * x + other))
        if r == 3 and i % 4 < 2:
            send(GRAD, part, part, a_recv.at[1, i, 0], at_depth(2 * right + core))
        if r == 1 and i % 4 >= 2:
            send(GRAD, part, part, a_recv.at[1, i, 0], at_depth(2 * left + core))

    def group(r, i):
        s = source[r]
        arrived(token_rows(s, i, other), a_recv.at[r - 1, i, 1])
        q, h, count, i = order[i % 4], i // 4, part_rows, i % 4
        if i in SPLIT:
            tokens = gbuf[s, q, :, h]
        else:
            tokens, count = gbuf[s, q], chunk
        part = times_weight(tokens.reshape(2 * count, features))
        low, high = part[:count], part[count:]
        rows = pl.ds(h * count, count)
        if i == 0:
            csend[r, 0, 0, rows] = low.astype(bf16)
            csend[r, 0, 1, rows] = high.astype(bf16)
            to_col(r, 0, 0, rows)
            to_col(r, 0, 1, rows)
        elif i == 1:
            csend[r, 1, 0, rows] = high.astype(bf16)
            keep[r, 0, rows] = low
            to_col(r, 1, 0, rows)
        elif i == 2:
            csend[r, 1, 1, rows] = low.astype(bf16)
            keep[r, 1, rows] = high
            to_col(r, 1, 1, rows)
        else:
            keep_own[r, 0, rows] = low
            keep_own[r, 1, rows] = high

    def combine(r, way):
        if r == 0:
            way = (core, other)[way]
        arrived(crecv.at[r, 0, way], c_recv.at[r, way])
        csend[r, 2, way] = (keep[r, way] + crecv[r, 0, way].astype(f32)).astype(bf16)
        to_col(r, 2, way)

    seen = set()

    def pre_arrived(r, i):
        s, rest = source[r], int(i < 3)
        if (r, rest) not in seen:
            seen.add((r, rest))
            chunks = pl.ds(0, 3 if rest else 1)
            arrived(pbuf.at[s, chunks, 0] if r == 0 else pbuf.at[s, chunks], p_recv.at[r, rest])

    def finish(r):
        arrived(crecv.at[r, pl.ds(1, 2)], c_recv.at[r, 2])
        pre_arrived(r, 3)
        s = source[r]
        for k in (0, 1):
            total = keep_own[r, k] + crecv[r, 2, k].astype(f32) + crecv[r, 1, 1 - k].astype(f32)
            dsend[r, k] = (total * gelu_slope(pbuf[s, col, k].astype(f32))).astype(bf16)
        mine = go.at[col, :, hidden(dep)]
        if r == 0:
            send(SHARE, dsend.at[0, other], mine, d_recv.at[0], at_depth(2 * x + other))
            local.append(pltpu.make_async_copy(dsend.at[0, core], mine, out_sem.at[0]))
            local[-1].start()
        else:
            for k in (0, 1):
                send(SHARE, dsend.at[r, k], mine, d_recv.at[4 - r], at_depth(2 * s + k))

    def piece(c, j):
        return go.at[c, :, hidden(j)]

    def e_own(r):
        s = source[r]
        if r == 0:
            arrived(piece(col, 2 * x + other), d_recv.at[0])
            local.pop(0).wait()
        else:
            arrived(dsend.at[r], d_recv.at[r])
        for flip in (0, 1):
            for k in (0, 1):
                part = piece(col, 2 * s + k)
                send(SPREAD, part, part, e_recv.at[r, 2 if flip else k], at_col((up, down)[k ^ flip]))

    def e_forward(r):
        for k, (frm, to) in enumerate(((down, up), (up, down))):
            part = piece(frm, 2 * source[r] + k)
            arrived(part, e_recv.at[r, k])
            send(SPREAD, part, part, e_recv.at[r, 2], at_col(to))

    def e_rest(r):
        arrived(crecv.at[r, pl.ds(0, 2)], e_recv.at[r, 2])

    def activate(r, i):
        pre_arrived(r, i)
        s, q = source[r], order[i]
        pre = pbuf[s, q].reshape(2 * chunk, wide).astype(f32)
        place = pl.ds(pl.multiple_of((4 * s + q) * 2 * chunk, 128), 2 * chunk)
        act_t[:, place] = gelu_value(pre).astype(bf16).T

    def weight_grad(r, n):
        s, cols = source[r], pl.ds(n * 512, 512)
        span = 8 * chunk
        part = jnp.dot(
            act_t[:, pl.ds(pl.multiple_of(s * span, 128), span)],
            gbuf[s, :, :, :, :, cols].reshape(span, 512),
            preferred_element_type=f32,
        )
        if r == 0:
            gw_sum[:, cols] = part
        elif r == 2:
            gw_buf[:, cols] = (gw_sum[:, cols] + part).astype(bf16)
            local.append(pltpu.make_async_copy(gw_buf.at[:, cols], gw.at[:, cols], out_sem.at[1 + n]))
            local[-1].start()
        else:
            gw_sum[:, cols] += part

    arrived(gbuf.at[x, order[0], other], s_recv.at[0])
    far_part(other)
    to_col(0, 0, other)
    arrived(gbuf.at[x, pl.ds(0, 3), other], s_recv.at[1])
    own_part(other)
    to_col(0, 1, core)

    steps = dict(
        X=from_x, G=group, C=combine, F=finish, O=e_own, W=e_forward, R=e_rest, A=activate, M=weight_grad,
        P=send_pre,
    )
    for name, *numbers in PLAN:
        steps[name](*numbers)
    every_grad = gbuf.reshape(64, part_rows, features)
    arrived(every_grad.at[pl.ds(0, 56)], sent.at[GRAD])
    arrived(pbuf.reshape(32, chunk, wide).at[pl.ds(0, 28)], sent.at[PRE])
    arrived(crecv, sent.at[SUM])
    arrived(dsend.reshape(8, chunk, wide).at[pl.ds(0, 7)], sent.at[SHARE])
    arrived(crecv, sent.at[SPREAD])
    for copy in local:
        copy.wait()


def write_results(go, gw, go_out, gw_out, sem):
    copies = []
    for n, (src, dst) in enumerate(((go, go_out), (gw, gw_out))):
        rows = src.shape[0] // 2
        for i in range(2):
            part = pl.ds(i * rows, rows)
            copies.append(pltpu.make_async_copy(src.at[part], dst.at[part], sem.at[n, i]))
    for copy in copies:
        copy.start()
    for copy in copies:
        copy.wait()


def on_device(grad_out, pre_act, down_weight):
    tokens, features = grad_out.shape
    hidden = pre_act.shape[1]
    wide = down_weight.shape[0]
    chunk = tokens // 4
    any_spec = pl.BlockSpec(memory_space=pl.ANY)
    dma = pltpu.SemaphoreType.DMA
    operands = (grad_out.reshape(4, 2, chunk // 2, features), pre_act.reshape(4, chunk, hidden), down_weight)
    grad_pre, grad_weight = pl.pallas_call(
        kernel,
        out_shape=(
            jax.ShapeDtypeStruct((4, chunk, hidden), bf16),
            jax.ShapeDtypeStruct((wide, features), bf16),
        ),
        in_specs=[any_spec] * 3,
        out_specs=(any_spec, any_spec),
        scratch_shapes=[
            pltpu.VMEM((4, 4, 2, 2, chunk // 2, features), bf16),
            pltpu.VMEM((4, 4, 2, chunk, wide), bf16),
            pltpu.VMEM((wide, features), bf16),
            pltpu.VMEM((2, 4, chunk, wide), f32),
            pltpu.VMEM((4, 3, 2, chunk, wide), bf16),
            pltpu.VMEM((4, 3, 2, chunk, wide), bf16),
            pltpu.VMEM((4, 2, chunk, wide), f32),
            pltpu.VMEM((4, 2, chunk, wide), f32),
            pltpu.VMEM((4, 2, chunk, wide), bf16),
            pltpu.VMEM((wide, 32 * chunk), bf16),
            pltpu.VMEM((wide, features), f32),
            pltpu.VMEM((wide, features), bf16),
            dma((3,)), dma((4,)), dma((2,)), dma((3, 5, 2)), dma((4, 2)), dma((4, 3)), dma((4,)), dma((4, 3)), dma((5,)),
        ],
        compiler_params=pltpu.CompilerParams(
            collective_id=0, has_side_effects=True, vmem_limit_bytes=44 * 1024 * 1024
        ),
    )(*(pltpu.with_memory_space_constraint(operand, pltpu.HBM) for operand in operands))
    return pl.pallas_call(
        write_results,
        out_shape=(
            jax.ShapeDtypeStruct((tokens, hidden), bf16),
            jax.ShapeDtypeStruct((wide, features), bf16),
        ),
        in_specs=[any_spec] * 2,
        out_specs=(any_spec, any_spec),
        scratch_shapes=[dma((2, 2))],
        compiler_params=pltpu.CompilerParams(vmem_limit_bytes=1024 * 1024),
    )(grad_pre.reshape(tokens, hidden), grad_weight)


def solution(mesh):
    placed = (P("depth", "col"), P("depth", "row"), P(("row", "depth"), "col"))
    return jax.shard_map(
        on_device,
        mesh=mesh,
        in_specs=placed,
        out_specs=(P("depth", "row"), P(("row", "depth"), "col")),
        check_vma=False,
    )
```

```python
import jax
import jax.numpy as jnp
from jax import lax
from jax.experimental import pallas as pl
from jax.experimental.pallas import tpu as pltpu
from jax.sharding import PartitionSpec as P

sqrt_two_pi = 0.7978845608028654
cubic_coeff = 0.044715
MESH = pl.DeviceIdType.MESH
bf16, f32 = jnp.bfloat16, jnp.float32


def gelu_value(preact):
    tangent = jnp.tanh(sqrt_two_pi * (preact + cubic_coeff * preact * preact * preact))
    return 0.5 * preact * (1.0 + tangent)


def gelu_slope(preact):
    tangent = jnp.tanh(sqrt_two_pi * (preact + cubic_coeff * preact * preact * preact))
    inner = sqrt_two_pi * (1.0 + 3.0 * cubic_coeff * preact * preact)
    return 0.5 * (1.0 + tangent) + 0.5 * preact * (1.0 - tangent * tangent) * inner


SPLIT = (0,)

PLAN = [
    ("X", 1, 0), ("X", 3, 0), ("G", 3, 0), ("C", 0, 0), ("C", 0, 1), ("A", 0, 3), ("X", 3, 4), ("G", 1, 0), ("X",
    1, 4), ("G", 3, 4), ("X", 1, 2), ("G", 1, 4), ("X", 3, 1), ("G", 1, 2), ("G", 3, 1), ("P", 3, 3), ("F", 0),
    ("O", 0), ("X", 1, 1), ("G", 1, 1), ("C", 1, 1), ("A", 0, 1), ("X", 3, 2), ("X", 1, 3), ("P", 3, 1), ("G", 3,
    2), ("C", 1, 0), ("X", 3, 3), ("P", 0, 3), ("C", 3, 0), ("C", 3, 1), ("A", 0, 2), ("G", 1, 3), ("A", 0, 0),
    ("X", 2, 4), ("X", 2, 0), ("G", 2, 0), ("G", 2, 4), ("X", 2, 2), ("P", 2, 3), ("W", 0), ("X", 2, 1), ("F", 1),
    ("G", 2, 2), ("P", 3, 2), ("M", 0, 1), ("G", 2, 1), ("G", 3, 3), ("F", 3), ("C", 2, 1), ("P", 2, 1), ("X", 2,
    3), ("P", 1, 3), ("P", 1, 1), ("C", 2, 0), ("P", 0, 1), ("G", 2, 3), ("O", 3), ("F", 2), ("O", 1), ("A", 1,
    2), ("A", 1, 0), ("M", 0, 0), ("W", 3), ("M", 0, 2), ("A", 3, 3), ("A", 1, 1), ("P", 2, 2), ("A", 3, 1), ("O",
    2), ("A", 2, 3), ("P", 0, 2), ("A", 3, 0), ("A", 3, 2), ("W", 1), ("A", 1, 3), ("P", 1, 2), ("W", 2), ("R",
    3), ("M", 1, 1), ("A", 2, 2), ("M", 3, 0), ("A", 2, 0), ("M", 1, 2), ("M", 1, 0), ("M", 3, 2), ("A", 2, 1),
    ("M", 2, 0), ("M", 2, 2), ("M", 3, 1), ("M", 2, 1), ("R", 2), ("R", 0), ("R", 1),
]


def kernel(
    g_hbm, p_hbm, w_hbm, go, gw,
    gbuf, pbuf, wbuf, first, csend, crecv, keep, keep_own, dsend, act_t, gw_sum, gw_buf,
    load_sem, out_sem, s_recv, a_recv, p_recv, c_recv, d_recv, e_recv, sent,
):
    row, col, dep = lax.axis_index("row"), lax.axis_index("col"), lax.axis_index("depth")
    x, core = dep // 2, dep % 2
    other = 1 - core
    part_rows, features = g_hbm.shape[2:]
    chunk = 2 * part_rows
    wide = wbuf.shape[0]
    right, left, far = (x + 1) % 4, (x + 3) % 4, (x + 2) % 4
    up, down = (col + 1) % 4, (col + 3) % 4
    order = [(col + 2) % 4, up, down, col]
    source = {0: x, 1: right, 2: far, 3: left}
    local = []

    def at_depth(d):
        return (row, col, d)

    def at_col(c):
        return (row, c, dep)

    GRAD, PRE, SUM, SHARE, SPREAD = range(5)

    def send(kind, src, dst, recv_sem, device):
        pltpu.make_async_remote_copy(
            src_ref=src, dst_ref=dst, send_sem=sent.at[kind], recv_sem=recv_sem, device_id=device, device_id_type=MESH
        ).start()

    def arrived(dst, recv_sem):
        pltpu.make_async_copy(dst, dst, recv_sem).wait()

    def hidden(d):
        return pl.ds(pl.multiple_of(d * wide, 128), wide)

    def times_weight(rows):
        return lax.dot_general(rows, wbuf[...], (((1,), (1,)), ((), ())), preferred_element_type=f32)

    barrier = pltpu.get_barrier_semaphore()
    for c in (up, down):
        pl.semaphore_signal(barrier, inc=1, device_id=at_col(c), device_id_type=MESH)
    for t in range(1, 8):
        pl.semaphore_signal(barrier, inc=1, device_id=at_depth((dep + t) % 8), device_id_type=MESH)
    loads = [
        pltpu.make_async_copy(w_hbm, wbuf, load_sem.at[0]),
        pltpu.make_async_copy(g_hbm, gbuf.at[x, :, core], load_sem.at[1]),
        pltpu.make_async_copy(p_hbm.at[:, :, hidden(dep)], pbuf.at[x, :, core], load_sem.at[2]),
    ]
    for copy in loads:
        copy.start()
    loads[0].wait()
    loads[1].wait()

    def own_part(k):
        rows = gbuf[x, :, k].reshape(4 * chunk, features)
        first[k] = times_weight(rows).reshape(4, chunk, wide)
        csend[0, 1, 1 - k] = first[k, (col + 3 + 2 * k) % 4].astype(bf16)
        keep[0, k] = first[k, (col + 1 + 2 * k) % 4]
        keep_own[0, k] = first[k, col]

    def far_part(k):
        csend[0, 0, k] = times_weight(gbuf[x, order[0], k].reshape(chunk, features)).astype(bf16)

    own_part(core)
    csend[0, 0, core] = first[core, order[0]].astype(bf16)
    loads[2].wait()
    pl.semaphore_wait(barrier, 9)

    def to_col(r, kind, way, rows=slice(None)):
        sem = c_recv.at[r, way] if kind == 0 else c_recv.at[r, 2]
        src, dst = csend.at[r, kind, way, rows], crecv.at[r, kind, way, rows]
        send(SUM, src, dst, sem, at_col((col + 1 + 2 * way) % 4))

    def token_rows(s, i, c):
        whole = gbuf.at[s, order[i % 4], c]
        return whole.at[i // 4] if i % 4 in SPLIT else whole

    def send_grad(i, r, d):
        mine = token_rows(x, i, core)
        send(GRAD, mine, mine, a_recv.at[r - 1, i, 0], at_depth(d))

    def send_pre(i, t):
        q = order[i]
        sem = p_recv.at[(4 - t) % 4, 0 if i == 3 else 1]
        for d in (2 * ((x + t) % 4) + core, 2 * ((x + t) % 4) + other)[0 if t else 1 :]:
            send(PRE, p_hbm.at[q, :, hidden(d)], pbuf.at[x, q, core], sem, at_depth(d))

    send_grad(0, 3, 2 * right + core)
    send_grad(0, 1, 2 * left + core)
    to_col(0, 0, core)
    to_col(0, 1, other)
    for i, q in enumerate(order):
        mine = gbuf.at[x, q, core]
        send(GRAD, mine, mine, s_recv.at[min(i, 1)], at_depth(2 * x + other))
    for i, j in ((0, 0), (1, 2), (2, 1), (3, 3)):
        for h in (0, 1):
            if h == 1 and i in SPLIT or h == 0 and i != 0:
                send_grad(i + 4 * h, 3, 2 * right + core)
            if h == 1 and j in SPLIT or h == 0 and j != 0:
                send_grad(j + 4 * h, 1, 2 * left + core)
    for i in (3, 0, 1, 2):
        send_pre(i, 0)

    def from_x(r, i):
        part, sem = token_rows(source[r], i, core), a_recv.at[r - 1, i]
        arrived(part, sem.at[0])
        send(GRAD, part, part, sem.at[1], at_depth(2 * x + other))
        if r == 3 and i % 4 < 2:
            send(GRAD, part, part, a_recv.at[1, i, 0], at_depth(2 * right + core))
        if r == 1 and i % 4 >= 2:
            send(GRAD, part, part, a_recv.at[1, i, 0], at_depth(2 * left + core))

    def group(r, i):
        s = source[r]
        arrived(token_rows(s, i, other), a_recv.at[r - 1, i, 1])
        q, h, count, i = order[i % 4], i // 4, part_rows, i % 4
        if i in SPLIT:
            tokens = gbuf[s, q, :, h]
        else:
            tokens, count = gbuf[s, q], chunk
        part = times_weight(tokens.reshape(2 * count, features))
        low, high = part[:count], part[count:]
        rows = pl.ds(h * count, count)
        if i == 0:
            csend[r, 0, 0, rows] = low.astype(bf16)
            csend[r, 0, 1, rows] = high.astype(bf16)
            to_col(r, 0, 0, rows)
            to_col(r, 0, 1, rows)
        elif i == 1:
            csend[r, 1, 0, rows] = high.astype(bf16)
            keep[r, 0, rows] = low
            to_col(r, 1, 0, rows)
        elif i == 2:
            csend[r, 1, 1, rows] = low.astype(bf16)
            keep[r, 1, rows] = high
            to_col(r, 1, 1, rows)
        else:
            keep_own[r, 0, rows] = low
            keep_own[r, 1, rows] = high

    def combine(r, way):
        if r == 0:
            way = (core, other)[way]
        arrived(crecv.at[r, 0, way], c_recv.at[r, way])
        csend[r, 2, way] = (keep[r, way] + crecv[r, 0, way].astype(f32)).astype(bf16)
        to_col(r, 2, way)

    seen = set()

    def pre_arrived(r, i):
        s, rest = source[r], int(i < 3)
        if (r, rest) not in seen:
            seen.add((r, rest))
            chunks = pl.ds(0, 3 if rest else 1)
            arrived(pbuf.at[s, chunks, 0] if r == 0 else pbuf.at[s, chunks], p_recv.at[r, rest])

    def finish(r):
        arrived(crecv.at[r, pl.ds(1, 2)], c_recv.at[r, 2])
        pre_arrived(r, 3)
        s = source[r]
        for k in (0, 1):
            total = keep_own[r, k] + crecv[r, 2, k].astype(f32) + crecv[r, 1, 1 - k].astype(f32)
            dsend[r, k] = (total * gelu_slope(pbuf[s, col, k].astype(f32))).astype(bf16)
        mine = go.at[col, :, hidden(dep)]
        if r == 0:
            send(SHARE, dsend.at[0, other], mine, d_recv.at[0], at_depth(2 * x + other))
            local.append(pltpu.make_async_copy(dsend.at[0, core], mine, out_sem.at[0]))
            local[-1].start()
        else:
            for k in (0, 1):
                send(SHARE, dsend.at[r, k], mine, d_recv.at[4 - r], at_depth(2 * s + k))

    def piece(c, j):
        return go.at[c, :, hidden(j)]

    def e_own(r):
        s = source[r]
        if r == 0:
            arrived(piece(col, 2 * x + other), d_recv.at[0])
            local.pop(0).wait()
        else:
            arrived(dsend.at[r], d_recv.at[r])
        for flip in (0, 1):
            for k in (0, 1):
                part = piece(col, 2 * s + k)
                send(SPREAD, part, part, e_recv.at[r, 2 if flip else k], at_col((up, down)[k ^ flip]))

    def e_forward(r):
        for k, (frm, to) in enumerate(((down, up), (up, down))):
            part = piece(frm, 2 * source[r] + k)
            arrived(part, e_recv.at[r, k])
            send(SPREAD, part, part, e_recv.at[r, 2], at_col(to))

    def e_rest(r):
        arrived(crecv.at[r, pl.ds(0, 2)], e_recv.at[r, 2])

    def activate(r, i):
        pre_arrived(r, i)
        s, q = source[r], order[i]
        pre = pbuf[s, q].reshape(2 * chunk, wide).astype(f32)
        place = pl.ds(pl.multiple_of((4 * s + q) * 2 * chunk, 128), 2 * chunk)
        act_t[:, place] = gelu_value(pre).astype(bf16).T

    def weight_grad(r, n):
        s, cols = source[r], pl.ds(n * 512, 512)
        span = 8 * chunk
        part = jnp.dot(
            act_t[:, pl.ds(pl.multiple_of(s * span, 128), span)],
            gbuf[s, :, :, :, :, cols].reshape(span, 512),
            preferred_element_type=f32,
        )
        if r == 0:
            gw_sum[:, cols] = part
        elif r == 2:
            gw_buf[:, cols] = (gw_sum[:, cols] + part).astype(bf16)
            local.append(pltpu.make_async_copy(gw_buf.at[:, cols], gw.at[:, cols], out_sem.at[1 + n]))
            local[-1].start()
        else:
            gw_sum[:, cols] += part

    arrived(gbuf.at[x, order[0], other], s_recv.at[0])
    far_part(other)
    to_col(0, 0, other)
    arrived(gbuf.at[x, pl.ds(0, 3), other], s_recv.at[1])
    own_part(other)
    to_col(0, 1, core)

    steps = dict(
        X=from_x, G=group, C=combine, F=finish, O=e_own, W=e_forward, R=e_rest, A=activate, M=weight_grad,
        P=send_pre,
    )
    for name, *numbers in PLAN:
        steps[name](*numbers)
    every_grad = gbuf.reshape(64, part_rows, features)
    arrived(every_grad.at[pl.ds(0, 56)], sent.at[GRAD])
    arrived(pbuf.reshape(32, chunk, wide).at[pl.ds(0, 28)], sent.at[PRE])
    arrived(crecv, sent.at[SUM])
    arrived(dsend.reshape(8, chunk, wide).at[pl.ds(0, 7)], sent.at[SHARE])
    arrived(crecv, sent.at[SPREAD])
    for copy in local:
        copy.wait()


def write_results(go, gw, go_out, gw_out, sem):
    copies = [pltpu.make_async_copy(go, go_out, sem.at[0]), pltpu.make_async_copy(gw, gw_out, sem.at[1])]
    for copy in copies:
        copy.start()
    for copy in copies:
        copy.wait()


def on_device(grad_out, pre_act, down_weight):
    tokens, features = grad_out.shape
    hidden = pre_act.shape[1]
    wide = down_weight.shape[0]
    chunk = tokens // 4
    any_spec = pl.BlockSpec(memory_space=pl.ANY)
    dma = pltpu.SemaphoreType.DMA
    operands = (grad_out.reshape(4, 2, chunk // 2, features), pre_act.reshape(4, chunk, hidden), down_weight)
    grad_pre, grad_weight = pl.pallas_call(
        kernel,
        out_shape=(
            jax.ShapeDtypeStruct((4, chunk, hidden), bf16),
            jax.ShapeDtypeStruct((wide, features), bf16),
        ),
        in_specs=[any_spec] * 3,
        out_specs=(any_spec, any_spec),
        scratch_shapes=[
            pltpu.VMEM((4, 4, 2, 2, chunk // 2, features), bf16),
            pltpu.VMEM((4, 4, 2, chunk, wide), bf16),
            pltpu.VMEM((wide, features), bf16),
            pltpu.VMEM((2, 4, chunk, wide), f32),
            pltpu.VMEM((4, 3, 2, chunk, wide), bf16),
            pltpu.VMEM((4, 3, 2, chunk, wide), bf16),
            pltpu.VMEM((4, 2, chunk, wide), f32),
            pltpu.VMEM((4, 2, chunk, wide), f32),
            pltpu.VMEM((4, 2, chunk, wide), bf16),
            pltpu.VMEM((wide, 32 * chunk), bf16),
            pltpu.VMEM((wide, features), f32),
            pltpu.VMEM((wide, features), bf16),
            dma((3,)), dma((4,)), dma((2,)), dma((3, 5, 2)), dma((4, 2)), dma((4, 3)), dma((4,)), dma((4, 3)), dma((5,)),
        ],
        compiler_params=pltpu.CompilerParams(
            collective_id=0, has_side_effects=True, vmem_limit_bytes=44 * 1024 * 1024
        ),
    )(*(pltpu.with_memory_space_constraint(operand, pltpu.HBM) for operand in operands))
    return pl.pallas_call(
        write_results,
        out_shape=(
            jax.ShapeDtypeStruct((tokens, hidden), bf16),
            jax.ShapeDtypeStruct((wide, features), bf16),
        ),
        in_specs=[any_spec] * 2,
        out_specs=(any_spec, any_spec),
        scratch_shapes=[dma((2,))],
        compiler_params=pltpu.CompilerParams(vmem_limit_bytes=1024 * 1024),
    )(grad_pre.reshape(tokens, hidden), grad_weight)


def solution(mesh):
    placed = (P("depth", "col"), P("depth", "row"), P(("row", "depth"), "col"))
    return jax.shard_map(
        on_device,
        mesh=mesh,
        in_specs=placed,
        out_specs=(P("depth", "row"), P(("row", "depth"), "col")),
        check_vma=False,
    )
```
